256 devices in a mesh: outer: 8 (over z_hi, core), inner: 8 (over x, z_lo), head: 4 (over y).
Axes of the slice: x: 4, y: 4, z: 8 (z_hi: 4, z_lo: 2; z = z_hi * 2 + z_lo), core: 2. Of those that a mesh axis runs over, the one named last changes fastest.
Arguments:
- stored_query_rows: bfloat16 [16384, 32, 128], P(('outer', 'inner'), 'head'), may hold values from -12 to 12
- stored_key_rows: bfloat16 [16384, 8, 128], P(('outer', 'inner'), 'head'), may hold values from -12 to 12
- stored_value_rows: bfloat16 [16384, 8, 128], P(('outer', 'inner'), 'head'), may hold values from -6 to 6
- span_order: int32 [128], replicated, may hold values from 0 to 127, each once
Outputs:
- attended: bfloat16 [16384, 32, 128], P(('outer', 'inner'), 'head')
The draws below stay inside these ranges and needn't reach their ends.
Inputs may be any that keep to these rules, and one draw needn't show every extreme that they name: `span_order`: a permutation of the sequence's 128 blocks of 128 tokens.
All inputs are finite; a program needn't handle non-finite values.
Results may differ from the reference program's by a relative error of at most 0.0075.
Values may be sent and summed in bfloat16 or wider, within the bound.
A program may use at most 128 MiB of HBM per device.

```python
import math
import jax
import jax.numpy as jnp
from jax import lax

QUERY_HEADS = 32
KEY_VALUE_HEADS = 8
HEAD_DIMENSION = 128
BLOCK_TOKENS = 128
STORED_BLOCKS = 128
SEQUENCE_TOKENS = 16384


def draw_stored_query_rows(key, part):
    value_matrix = jnp.clip(jax.random.normal(jax.random.fold_in(key, 11), (SEQUENCE_TOKENS, QUERY_HEADS, HEAD_DIMENSION), jnp.float32), -6.0, 6.0)
    return value_matrix.astype(jnp.bfloat16)


def draw_stored_key_rows(key, part):
    value_matrix = jnp.clip(jax.random.normal(jax.random.fold_in(key, 12), (SEQUENCE_TOKENS, KEY_VALUE_HEADS, HEAD_DIMENSION), jnp.float32), -6.0, 6.0)
    return value_matrix.astype(jnp.bfloat16)


def block_levels(key, dims, shards, low, largest):
    level = 1.0
    for position, shards_of in shards:
        draws = jax.random.uniform(jax.random.fold_in(jax.random.fold_in(key, 6), position), (shards_of,), jnp.float32, low / len(shards), largest / len(shards))
        level = level * jnp.repeat(jnp.exp(draws), dims[position] // shards_of).reshape((-1,) + (1,) * (len(dims) - 1 - position))
    return level


def bell_draw(stream_key, dims, width, reach, pieces=(), held_as=jnp.bfloat16):
    entries = jax.random.normal(stream_key, dims, jnp.float32) * width
    if len(pieces) > 0:
        entries = block_levels(stream_key, dims, pieces, -0.22, 0.18) * entries
    return jnp.clip(entries, min=-reach, max=reach).astype(held_as)


def setup_inputs(seed: int = 0) -> dict:
    key_of = jax.random.split(jax.random.key(seed), 5)
    stored_query_rows = draw_stored_query_rows(jax.random.fold_in(key_of[4], 71), 0)
    stored_key_rows = draw_stored_key_rows(jax.random.fold_in(key_of[4], 71), 0)
    stored_value_rows = bell_draw(key_of[2], (SEQUENCE_TOKENS, KEY_VALUE_HEADS, HEAD_DIMENSION), 1.0, 6.0, ((0, 64), (1, 4)))
    span_order = jax.random.permutation(key_of[3], STORED_BLOCKS).astype(jnp.int32)
    return {"stored_query_rows": stored_query_rows, "stored_key_rows": stored_key_rows, "stored_value_rows": stored_value_rows, "span_order": span_order}


def attend_block(carry, query_tile, key_tile, value_tile, allowed, score_scale):
    run_max, run_sum, run_acc = carry
    scores = jnp.einsum('ghqa,kga->ghqk', query_tile.astype(jnp.float32), key_tile.astype(jnp.float32)) * score_scale
    scores = jnp.where(allowed[None, None], scores, -1e+30)
    new_max = jnp.maximum(run_max, lax.optimization_barrier(jnp.max(scores, axis=-1)))
    weights = jnp.where(allowed[None, None], jnp.exp(scores - new_max[..., None]), 0.0)
    rescale = jnp.exp(run_max - new_max)
    new_sum = run_sum * rescale + lax.optimization_barrier(jnp.sum(weights, axis=-1))
    rounded = lax.optimization_barrier(weights.astype(jnp.bfloat16)).astype(jnp.float32)
    added = jnp.einsum('ghqk,kga->ghqa', rounded, value_tile.astype(jnp.float32))
    return (new_max, new_sum, run_acc * rescale[..., None] + added)

def reference(stored_query_rows, stored_key_rows, stored_value_rows, span_order):
    heads_per_group = QUERY_HEADS // KEY_VALUE_HEADS
    inverse_permutation = jnp.zeros((STORED_BLOCKS,), jnp.int32).at[span_order].set(jnp.arange(STORED_BLOCKS, dtype=jnp.int32))
    query_in_order = stored_query_rows.reshape(STORED_BLOCKS, BLOCK_TOKENS, KEY_VALUE_HEADS, heads_per_group, HEAD_DIMENSION)[inverse_permutation].transpose(0, 2, 3, 1, 4)
    key_in_order = stored_key_rows.reshape(STORED_BLOCKS, BLOCK_TOKENS, KEY_VALUE_HEADS, HEAD_DIMENSION)[inverse_permutation]
    value_in_order = stored_value_rows.reshape(STORED_BLOCKS, BLOCK_TOKENS, KEY_VALUE_HEADS, HEAD_DIMENSION)[inverse_permutation]
    score_scale = 1.0 / math.sqrt(HEAD_DIMENSION)
    offsets = jnp.arange(BLOCK_TOKENS, dtype=jnp.int32)

    def one_span(index):
        query_tile = query_in_order[index]

        def visit(block, carry):
            allowed = (block * BLOCK_TOKENS + offsets)[None, :] <= (index * BLOCK_TOKENS + offsets)[:, None]
            return attend_block(carry, query_tile, key_in_order[block], value_in_order[block], allowed, score_scale)
        initial_state = (jnp.full((KEY_VALUE_HEADS, heads_per_group, BLOCK_TOKENS), -1e+30, jnp.float32), jnp.zeros((KEY_VALUE_HEADS, heads_per_group, BLOCK_TOKENS), jnp.float32), jnp.zeros((KEY_VALUE_HEADS, heads_per_group, BLOCK_TOKENS, HEAD_DIMENSION), jnp.float32))
        run_max, run_sum, run_acc = lax.fori_loop(0, index + 1, visit, initial_state)
        return run_acc / run_sum[..., None]
    result = lax.map(one_span, jnp.arange(STORED_BLOCKS, dtype=jnp.int32))
    result = result[span_order]
    return result.transpose(0, 3, 1, 2, 4).reshape(SEQUENCE_TOKENS, QUERY_HEADS, HEAD_DIMENSION).astype(jnp.bfloat16)
```

```python
import math

import jax
import jax.numpy as jnp
from jax import lax
from jax.experimental import pallas as pl
from jax.experimental.pallas import tpu as pltpu
from jax.sharding import PartitionSpec as P

CHUNK = 512
ROW = 4
RING = 8
MESH = pl.DeviceIdType.MESH


def place():
    outer, inner = lax.axis_index("outer"), lax.axis_index("inner")
    return inner // 2, outer // 2 * 2 + inner % 2, outer % 2, lax.axis_index("head")


def device(x, z, c, y):
    return (z // 2 * 2 + c, x * 2 + z % 2, y)


def greet(peers):
    barrier = pltpu.get_barrier_semaphore()
    for peer in peers:
        pl.semaphore_signal(barrier, inc=1, device_id=peer, device_id_type=MESH)
    pl.semaphore_wait(barrier, len(peers))


def row_mates(x, z, c, y):
    steps = [(dx, dc) for dx in range(ROW) for dc in range(2) if (dx, dc) != (0, 0)]
    return steps, [device((x + dx) % ROW, z, (c + dc) % 2, y) for dx, dc in steps]


def gather_kernel(q_ref, kv_ref, q_all, kv_all, q_send, q_recv, x_send, x_recv, up_send, up_recv,
                  down_send, down_recv, core_send, core_recv, own_sem):
    x, z, c, y = place()
    steps, mates = row_mates(x, z, c, y)
    above, below = device(x, (z + 1) % RING, c, y), device(x, (z + RING - 1) % RING, c, y)
    partner = device(x, z, 1 - c, y)
    greet([*mates, above, below])

    def remote(src, dst, send, recv, to):
        return pltpu.make_async_remote_copy(
            src_ref=src, dst_ref=dst, send_sem=send, recv_sem=recv, device_id=to, device_id_type=MESH)

    started = []
    role = x % 2 * 2 + x // 2
    mine = kv_ref.at[role]
    keep_kv = pltpu.make_async_copy(mine, kv_all.at[c, z, x], own_sem.at[0])
    keep_q = pltpu.make_async_copy(q_ref.at[x % 2, c], q_all.at[x, c], own_sem.at[1])

    def pass_up(t, j, src):
        slot = kv_all.at[c, (z - t + RING) % RING, (x + j) % ROW]
        copy = remote(src, slot, up_send.at[t, j], up_recv.at[t, j], above)
        copy.start()
        started.append(copy)

    def pass_down(t, j, src):
        slot = kv_all.at[c, (z + t) % RING, (x + j) % ROW]
        copy = remote(src, slot, down_send.at[t, j], down_recv.at[t, j], below)
        copy.start()
        started.append(copy)

    def to_partner(r, j, src):
        slot = kv_all.at[c, (z + r) % RING, (x + j) % ROW]
        copy = remote(src, slot, core_send.at[r, j], core_recv.at[r, j], partner)
        copy.start()
        started.append(copy)

    pass_up(0, 0, mine)
    pass_down(0, 0, mine)
    for d in (1, 3, 2):
        to = (x + d) % ROW
        copy = remote(kv_ref.at[to % 2 * 2 + to // 2], kv_all.at[c, z, x], x_send.at[d], x_recv.at[d],
                      device(to, z, c, y))
        copy.start()
        started.append(copy)
    to_partner(0, 0, mine)
    keep_kv.start()
    keep_q.start()
    for n, (dx, dc) in enumerate(steps):
        to = (x + dx) % ROW
        copy = remote(q_ref.at[to % 2, (c + dc) % 2], q_all.at[x, c], q_send.at[n], q_recv.at[n], mates[n])
        copy.start()
        started.append(copy)

    def arrived(dst, recv):
        remote(dst, dst, x_send.at[0], recv, partner).wait_recv()

    for j in (1, 3, 2):
        slot = kv_all.at[c, z, (x + j) % ROW]
        arrived(slot, x_recv.at[ROW - j])
        pass_up(0, j, slot)
        pass_down(0, j, slot)
        to_partner(0, j, slot)
    for t in range(1, RING // 2 + 1):
        last = t == RING // 2
        for j in (0, 1, 3, 2):
            if not last or j in (0, 1):
                slot = kv_all.at[c, (z - t + RING) % RING, (x + j) % ROW]
                arrived(slot, up_recv.at[t - 1, j])
                if t < RING // 2 - 1 or (t == RING // 2 - 1 and j in (0, 1)):
                    pass_up(t, j, slot)
                to_partner((RING - t) % RING, j, slot)
            if not last or j in (2, 3):
                slot = kv_all.at[c, (z + t) % RING, (x + j) % ROW]
                arrived(slot, down_recv.at[t - 1, j])
                if t < RING // 2 - 1 or (t == RING // 2 - 1 and j in (2, 3)):
                    pass_down(t, j, slot)
                to_partner(t, j, slot)
    for n, (dx, dc) in enumerate(steps):
        arrived(q_all.at[(x + ROW - dx) % ROW, (c + dc) % 2], q_recv.at[n])
    for r in range(RING):
        for j in range(ROW):
            arrived(kv_all.at[1 - c, (z + r) % RING, (x + j) % ROW], core_recv.at[r, j])
    keep_kv.wait()
    keep_q.wait()
    for copy in started:
        copy.wait_send()


def gather(q, kv):
    sem = pltpu.SemaphoreType.DMA
    half_ring = RING // 2
    vmem = pl.BlockSpec(memory_space=pltpu.VMEM)
    return pl.pallas_call(
        gather_kernel,
        out_shape=(jax.ShapeDtypeStruct((ROW, 2, *q.shape[2:]), q.dtype),
                   jax.ShapeDtypeStruct((2, RING, ROW, *kv.shape[1:]), kv.dtype)),
        in_specs=[vmem, vmem],
        out_specs=(vmem, vmem),
        scratch_shapes=[
            sem((2 * ROW - 1,)), sem((2 * ROW - 1,)), sem((ROW,)), sem((ROW,)),
            sem((half_ring, ROW)), sem((half_ring, ROW)), sem((half_ring, ROW)), sem((half_ring, ROW)),
            sem((RING, ROW)), sem((RING, ROW)), sem((2,)),
        ],
        compiler_params=pltpu.CompilerParams(
            collective_id=0, has_side_effects=True, vmem_limit_bytes=32 * 1024 * 1024),
        cost_estimate=pl.CostEstimate(flops=0, bytes_accessed=20_000_000, transcendentals=0),
    )(q, kv)


def attend_kernel(half_ref, q_pos, k_pos, q_ref, kv_ref, o_ref, lse_ref,
                  k_sorted, v_sorted, v_turned, s_even, s_odd, acc, top, total):
    groups, _, each, piece, width = kv_ref.shape
    tiles, lanes, _ = q_ref.shape
    block = 2 * piece
    per_chunk = CHUNK // piece
    rate = math.log2(math.e) / math.sqrt(width)
    half = half_ref[0]

    def put(g, c):
        for b in range(each):
            at = pl.multiple_of(k_pos[g * each + b] * piece, piece)
            k_sorted[pl.ds(at, piece), :] = kv_ref[g, 0, b]
            v_sorted[pl.ds(at, piece), :] = kv_ref[g, 1, b]
        return c

    lax.fori_loop(0, groups, put, 0, unroll=2)

    def turn(g, c):
        at = pl.multiple_of(g * CHUNK, CHUNK)
        v_turned[:, pl.ds(at, CHUNK)] = v_sorted[pl.ds(at, CHUNK), :].T
        return c

    lax.fori_loop(0, groups * each * piece // CHUNK, turn, 0)

    def scores(j, t, out):
        at = pl.multiple_of(j * CHUNK, CHUNK)
        out[...] = lax.dot_general(
            k_sorted[pl.ds(at, CHUNK), :], q_ref[t], (((1,), (1,)), ((), ())),
            preferred_element_type=jnp.float32)

    def absorb(j, s):
        at = pl.multiple_of(j * CHUNK, CHUNK)
        old = top[...]
        new = jnp.maximum(old, jnp.max(s, axis=0, keepdims=True))
        p = jnp.exp2((s - new) * rate)
        fade = jnp.exp2((old - new) * rate)
        top[...] = new
        total[...] = total[...] * fade + jnp.sum(p, axis=0, keepdims=True)
        acc[...] = acc[...] * fade + jnp.dot(
            v_turned[:, pl.ds(at, CHUNK)], p.astype(jnp.bfloat16),
            preferred_element_type=jnp.float32)

    def tile(t, c):
        pos = q_pos[t]
        full = pos // per_chunk
        top[...] = jnp.full_like(top, -1e30)
        total[...] = jnp.zeros_like(total)
        acc[...] = jnp.zeros_like(acc)
        scores(0, t, s_even)

        def pair(h, c):
            scores(2 * h + 1, t, s_odd)
            absorb(2 * h, s_even[...])
            scores(2 * h + 2, t, s_even)
            absorb(2 * h + 1, s_odd[...])
            return c

        lax.fori_loop(0, full // 2, pair, 0)

        def last(s_buf):
            k_row = lax.broadcasted_iota(jnp.int32, (CHUNK, lanes), 0)
            k_at = (full * per_chunk + k_row // piece) * block + k_row % piece + half * piece
            q_row = lax.broadcasted_iota(jnp.int32, (CHUNK, lanes), 1)
            q_at = pos * block + q_row % block
            absorb(full, jnp.where(k_at <= q_at, s_buf[...], -2e30))

        @pl.when(full % 2 == 1)
        def _():
            scores(full, t, s_odd)
            absorb(full - 1, s_even[...])
            last(s_odd)

        @pl.when(full % 2 == 0)
        def _():
            last(s_even)

        weight = total[...]
        some = weight > 0
        weight = jnp.where(some, weight, 1.0)
        o_ref[t] = (acc[...] * (1.0 / weight)).T.astype(jnp.bfloat16)
        lse_ref[t] = jnp.where(some, top[...] * rate + jnp.log2(weight), -1e30)
        return c

    lax.fori_loop(0, tiles, tile, 0)


def attend(half, q_pos, k_pos, q, kv):
    tiles, lanes, width = q.shape
    groups, _, each, piece, _ = kv.shape
    keys = groups * each * piece
    smem = pl.BlockSpec(memory_space=pltpu.SMEM)
    vmem = pl.BlockSpec(memory_space=pltpu.VMEM)
    return pl.pallas_call(
        attend_kernel,
        out_shape=(jax.ShapeDtypeStruct(q.shape, jnp.bfloat16),
                   jax.ShapeDtypeStruct((tiles, 1, lanes), jnp.float32)),
        in_specs=[smem, smem, smem, vmem, vmem],
        out_specs=(vmem, vmem),
        scratch_shapes=[
            pltpu.VMEM((keys, width), jnp.bfloat16),
            pltpu.VMEM((keys, width), jnp.bfloat16),
            pltpu.VMEM((width, keys), jnp.bfloat16),
            pltpu.VMEM((CHUNK, lanes), jnp.float32),
            pltpu.VMEM((CHUNK, lanes), jnp.float32),
            pltpu.VMEM((width, lanes), jnp.float32),
            pltpu.VMEM((1, lanes), jnp.float32),
            pltpu.VMEM((1, lanes), jnp.float32),
        ],
        compiler_params=pltpu.CompilerParams(vmem_limit_bytes=48 * 1024 * 1024),
    )(half, q_pos, k_pos, q, kv)


def return_kernel(o_ref, lse_ref, o_all, lse_all, o_send, o_recv, l_send, l_recv, own_sem):
    x, z, c, y = place()
    steps, mates = row_mates(x, z, c, y)
    greet(mates)
    keep = [pltpu.make_async_copy(o_ref.at[x, c], o_all.at[x, c], own_sem.at[0]),
            pltpu.make_async_copy(lse_ref.at[x, c], lse_all.at[x, c], own_sem.at[1])]
    copies = []
    for n, (dx, dc) in enumerate(steps):
        to_x, to_c = (x + dx) % ROW, (c + dc) % 2
        for src, dst, send, recv in ((lse_ref, lse_all, l_send, l_recv), (o_ref, o_all, o_send, o_recv)):
            copy = pltpu.make_async_remote_copy(
                src_ref=src.at[to_x, to_c], dst_ref=dst.at[x, c], send_sem=send.at[n], recv_sem=recv.at[n],
                device_id=mates[n], device_id_type=MESH)
            copy.start()
            copies.append(copy)
    for copy in keep:
        copy.start()
    for copy in keep:
        copy.wait()
    for copy in copies:
        copy.wait()


def send_back(o, lse):
    sem = pltpu.SemaphoreType.DMA
    vmem = pl.BlockSpec(memory_space=pltpu.VMEM)
    n = 2 * ROW - 1
    return pl.pallas_call(
        return_kernel,
        out_shape=(jax.ShapeDtypeStruct(o.shape, o.dtype), jax.ShapeDtypeStruct(lse.shape, lse.dtype)),
        in_specs=[vmem, vmem],
        out_specs=(vmem, vmem),
        scratch_shapes=[sem((n,)), sem((n,)), sem((n,)), sem((n,)), sem((2,))],
        compiler_params=pltpu.CompilerParams(
            collective_id=1, has_side_effects=True, vmem_limit_bytes=32 * 1024 * 1024),
        cost_estimate=pl.CostEstimate(flops=0, bytes_accessed=20_000_000, transcendentals=0),
    )(o, lse)


def body(stored_query_rows, stored_key_rows, stored_value_rows, span_order):
    rows, heads, width = stored_query_rows.shape
    each = 2
    span = rows // each
    x, z, c, _ = place()
    q = stored_query_rows.reshape(each, span, 2, 2, 2, width).transpose(2, 3, 0, 4, 1, 5)
    q = q.reshape(2, 2, each, 2 * span, width)
    kv = jnp.stack([stored_key_rows, stored_value_rows])
    kv = kv.reshape(2, each, 2, span // 2, 2, width).transpose(4, 2, 0, 1, 3, 5)
    kv = kv.reshape(4, 2, each, span // 2, width)
    q_all, kv_all = gather(q, kv)

    order = span_order.reshape(RING // 2, 2, ROW, 2, each)
    k_pos = order.transpose(1, 0, 3, 2, 4).reshape(-1)
    in_row = lax.dynamic_index_in_dim(lax.dynamic_index_in_dim(order, z // 2, 0, False), z % 2, 2, False)
    q_pos = in_row.transpose(1, 0, 2).reshape(-1)
    half = jnp.reshape(x // 2, (1,)).astype(jnp.int32)
    o, lse = attend(half, q_pos, k_pos, q_all.reshape(2 * ROW * each, 2 * span, width),
                    kv_all.reshape(2 * RING * ROW, 2, each, span // 2, width))

    o, lse = send_back(o.reshape(ROW, 2, each, 2 * span, width), lse.reshape(ROW, 2, each, 1, 2 * span))
    o = o.reshape(2, 2, 2, each, 2, span, width)
    lse = lse.reshape(2, 2, 2, each, 2, span)
    top = jnp.max(lse, axis=0)
    weights = jnp.exp2(lse - top)
    share = weights / jnp.sum(weights, axis=0)
    result = jnp.sum(o.astype(jnp.float32) * share[..., None], axis=0).astype(jnp.bfloat16)
    return result.transpose(2, 4, 0, 1, 3, 5).reshape(rows, heads, width)


def solution(mesh):
    placed = (
        P(("outer", "inner"), "head", None),
        P(("outer", "inner"), "head", None),
        P(("outer", "inner"), "head", None),
        P(),
    )
    return jax.shard_map(
        body,
        mesh=mesh,
        in_specs=placed,
        out_specs=P(("outer", "inner"), "head", None),
        check_vma=False,
    )
```

```python
import math

import jax
import jax.numpy as jnp
from jax import lax
from jax.experimental import pallas as pl
from jax.experimental.pallas import tpu as pltpu
from jax.sharding import PartitionSpec as P

CHUNK = 1024
UNROLL = 4
ROW = 4
RING = 8
MESH = pl.DeviceIdType.MESH


def place():
    outer, inner = lax.axis_index("outer"), lax.axis_index("inner")
    return inner // 2, outer // 2 * 2 + inner % 2, outer % 2, lax.axis_index("head")


def device(x, z, c, y):
    return (z // 2 * 2 + c, x * 2 + z % 2, y)


def greet(peers):
    barrier = pltpu.get_barrier_semaphore()
    for peer in peers:
        pl.semaphore_signal(barrier, inc=1, device_id=peer, device_id_type=MESH)
    pl.semaphore_wait(barrier, len(peers))


def row_mates(x, z, c, y):
    steps = [(dx, dc) for dx in range(ROW) for dc in range(2) if (dx, dc) != (0, 0)]
    return steps, [device((x + dx) % ROW, z, (c + dc) % 2, y) for dx, dc in steps]


def gather_kernel(q_ref, kv_ref, q_all, kv_all, q_send, q_recv, x_send, x_recv, up_send, up_recv,
                  down_send, down_recv, core_send, core_recv, own_sem):
    x, z, c, y = place()
    steps, mates = row_mates(x, z, c, y)
    above, below = device(x, (z + 1) % RING, c, y), device(x, (z + RING - 1) % RING, c, y)
    partner = device(x, z, 1 - c, y)
    greet([*mates, above, below])

    def remote(src, dst, send, recv, to):
        return pltpu.make_async_remote_copy(
            src_ref=src, dst_ref=dst, send_sem=send, recv_sem=recv, device_id=to, device_id_type=MESH)

    started = []
    role = x % 2 * 2 + x // 2
    mine = kv_ref.at[role]
    keep_kv = pltpu.make_async_copy(mine, kv_all.at[c, z, x], own_sem.at[0])
    keep_q = pltpu.make_async_copy(q_ref.at[x % 2, c], q_all.at[x, c], own_sem.at[1])

    def pass_up(t, j, src):
        slot = kv_all.at[c, (z - t + RING) % RING, (x + j) % ROW]
        copy = remote(src, slot, up_send.at[t, j], up_recv.at[t, j], above)
        copy.start()
        started.append(copy)

    def pass_down(t, j, src):
        slot = kv_all.at[c, (z + t) % RING, (x + j) % ROW]
        copy = remote(src, slot, down_send.at[t, j], down_recv.at[t, j], below)
        copy.start()
        started.append(copy)

    def to_partner(r, j, src):
        slot = kv_all.at[c, (z + r) % RING, (x + j) % ROW]
        copy = remote(src, slot, core_send.at[r, j], core_recv.at[r, j], partner)
        copy.start()
        started.append(copy)

    pass_up(0, 0, mine)
    pass_down(0, 0, mine)
    for d in (1, 3, 2):
        to = (x + d) % ROW
        copy = remote(kv_ref.at[to % 2 * 2 + to // 2], kv_all.at[c, z, x], x_send.at[d], x_recv.at[d],
                      device(to, z, c, y))
        copy.start()
        started.append(copy)
    to_partner(0, 0, mine)
    keep_kv.start()
    keep_q.start()
    for n, (dx, dc) in enumerate(steps):
        to = (x + dx) % ROW
        copy = remote(q_ref.at[to % 2, (c + dc) % 2], q_all.at[x, c], q_send.at[n], q_recv.at[n], mates[n])
        copy.start()
        started.append(copy)

    def arrived(dst, recv):
        remote(dst, dst, x_send.at[0], recv, partner).wait_recv()

    for j in (1, 3, 2):
        slot = kv_all.at[c, z, (x + j) % ROW]
        arrived(slot, x_recv.at[ROW - j])
        pass_up(0, j, slot)
        pass_down(0, j, slot)
        to_partner(0, j, slot)
    for t in range(1, RING // 2 + 1):
        last = t == RING // 2
        for j in (0, 1, 3, 2):
            if not last or j in (0, 1):
                slot = kv_all.at[c, (z - t + RING) % RING, (x + j) % ROW]
                arrived(slot, up_recv.at[t - 1, j])
                if t < RING // 2 - 1 or (t == RING // 2 - 1 and j in (0, 1)):
                    pass_up(t, j, slot)
                to_partner((RING - t) % RING, j, slot)
            if not last or j in (2, 3):
                slot = kv_all.at[c, (z + t) % RING, (x + j) % ROW]
                arrived(slot, down_recv.at[t - 1, j])
                if t < RING // 2 - 1 or (t == RING // 2 - 1 and j in (2, 3)):
                    pass_down(t, j, slot)
                to_partner(t, j, slot)
    for n, (dx, dc) in enumerate(steps):
        arrived(q_all.at[(x + ROW - dx) % ROW, (c + dc) % 2], q_recv.at[n])
    for r in range(RING):
        for j in range(ROW):
            arrived(kv_all.at[1 - c, (z + r) % RING, (x + j) % ROW], core_recv.at[r, j])
    keep_kv.wait()
    keep_q.wait()
    for copy in started:
        copy.wait_send()


def gather(q, kv):
    sem = pltpu.SemaphoreType.DMA
    half_ring = RING // 2
    vmem = pl.BlockSpec(memory_space=pltpu.VMEM)
    return pl.pallas_call(
        gather_kernel,
        out_shape=(jax.ShapeDtypeStruct((ROW, 2, *q.shape[2:]), q.dtype),
                   jax.ShapeDtypeStruct((2, RING, ROW, *kv.shape[1:]), kv.dtype)),
        in_specs=[vmem, vmem],
        out_specs=(vmem, vmem),
        scratch_shapes=[
            sem((2 * ROW - 1,)), sem((2 * ROW - 1,)), sem((ROW,)), sem((ROW,)),
            sem((half_ring, ROW)), sem((half_ring, ROW)), sem((half_ring, ROW)), sem((half_ring, ROW)),
            sem((RING, ROW)), sem((RING, ROW)), sem((2,)),
        ],
        compiler_params=pltpu.CompilerParams(
            collective_id=0, has_side_effects=True, vmem_limit_bytes=32 * 1024 * 1024),
        cost_estimate=pl.CostEstimate(flops=0, bytes_accessed=20_000_000, transcendentals=0),
    )(q, kv)


def attend_kernel(half_ref, q_pos, k_pos, q_ref, kv_ref, o_ref, lse_ref,
                  k_sorted, v_sorted, v_turned, q_turned, p_bufs, acc, top):
    groups, _, each, piece, width = kv_ref.shape
    tiles, lanes, _ = q_ref.shape
    block = 2 * piece
    rate = math.log2(math.e) / math.sqrt(width)
    half = half_ref[0]

    def put(g, c):
        for b in range(each):
            at = pl.multiple_of(CHUNK + k_pos[g * each + b] * piece, piece)
            k_sorted[pl.ds(at, piece), :] = kv_ref[g, 0, b]
            v_sorted[pl.ds(at - CHUNK, piece), :] = kv_ref[g, 1, b]
        return c

    lax.fori_loop(0, groups, put, 0, unroll=4)
    first = k_sorted[CHUNK:CHUNK + piece, :]
    for u in range(0, CHUNK, piece):
        k_sorted[u:u + piece, :] = first
    pads = CHUNK // width
    extra = v_turned.shape[1] - width
    v_turned[:pads] = jnp.zeros((pads, *v_turned.shape[1:]), v_turned.dtype)
    v_turned[pads:, width:, :] = jnp.ones((v_turned.shape[0] - pads, extra, width), v_turned.dtype)

    def turn(g, c):
        at = pl.multiple_of(g * width, width)
        v_turned[pads + g, :width, :] = v_sorted[pl.ds(at, width), :].T
        return c

    lax.fori_loop(0, groups * each * piece // width, turn, 0, unroll=8)

    def twice(k):
        return jnp.concatenate([k, k], axis=1)

    k_row = lax.broadcasted_iota(jnp.int32, (block, lanes), 0)
    q_row = lax.broadcasted_iota(jnp.int32, (block, lanes), 1)
    lag = k_row // piece * block + k_row % piece - q_row % block

    def score(into, group, keys):
        at = pl.multiple_of(group * width, width)
        return jnp.dot(twice(k_sorted[pl.ds(at, keys), :]), q_turned[into], preferred_element_type=jnp.float32)

    def start(t, items):
        q = (q_ref[t].astype(jnp.float32) * rate).T
        high = q.astype(jnp.bfloat16)
        q_turned[t, :width, :] = high
        q_turned[t, width:, :] = (q - high.astype(jnp.float32)).astype(jnp.bfloat16)
        own = q_pos[t] // 2
        s = score(t, pads + own, block)
        s = jnp.where(lag <= q_pos[t] % 2 * block - half * piece, s, -2e30)
        peak = jnp.maximum(jnp.max(s, axis=0, keepdims=True), -1e30)
        early = jnp.max(score(t, 0, piece), axis=0, keepdims=True)
        peak = jnp.where(own > 0, jnp.maximum(peak, early), peak)
        top[t] = peak
        acc[t] = jnp.dot(v_turned[pads + own], jnp.exp2(s - peak).astype(jnp.bfloat16),
                         preferred_element_type=jnp.float32)
        return items + jnp.maximum((own + pads - 1) // pads, 1)

    items = lax.fori_loop(0, tiles, start, 0, unroll=4)
    q_turned[tiles] = jnp.zeros(q_turned.shape[1:], q_turned.dtype)
    top[tiles] = jnp.zeros(top.shape[1:], jnp.float32)
    acc[tiles] = jnp.zeros(acc.shape[1:], jnp.float32)

    def where_is(t, w):
        own = jnp.where(t < tiles, q_pos[jnp.minimum(t, tiles - 1)] // 2, 0)
        into = jnp.where(own > 0, t, tiles)
        group = jnp.maximum(own - w * pads, 0)
        return into, group, own <= (w + 1) * pads

    def values(group):
        return jnp.concatenate([v_turned[group + i] for i in range(pads)], axis=1)

    def weigh(into, group, slot):
        p_bufs[slot][...] = jnp.exp2(score(into, group, CHUNK) - top[into]).astype(jnp.bfloat16)

    def absorb(into, group, slot):
        acc[into] += jnp.dot(values(group), p_bufs[slot][...], preferred_element_type=jnp.float32)

    def steps(n, at):
        t, w = at
        for u in range(UNROLL):
            into, group, last = where_is(t, w)
            t, w = jnp.where(last, t + 1, t), jnp.where(last, 0, w + 1)
            ahead, ahead_group, _ = where_is(t, w)
            weigh(ahead, ahead_group, 1 - u % 2)
            absorb(into, group, u % 2)
        return t, w

    begin, begin_group, _ = where_is(jnp.int32(0), jnp.int32(0))
    weigh(begin, begin_group, 0)
    lax.fori_loop(0, (items + UNROLL - 1) // UNROLL, steps, (jnp.int32(0), jnp.int32(0)))

    def again(t, c):
        start(t, 0)
        own = q_pos[t] // 2

        def window(w, c):
            group = own - w * pads
            s = score(t, group, CHUNK)
            old = top[t]
            new = jnp.maximum(old, jnp.max(s, axis=0, keepdims=True))
            top[t] = new
            acc[t] = acc[t] * jnp.exp2(old - new) + jnp.dot(
                values(group), jnp.exp2(s - new).astype(jnp.bfloat16), preferred_element_type=jnp.float32)
            return c

        return lax.fori_loop(0, (own + pads - 1) // pads, window, c)

    most = acc[0, width:width + 8, :]
    for t in range(1, tiles):
        most = jnp.maximum(most, acc[t, width:width + 8, :])

    @pl.when(jnp.logical_not(jnp.max(most) < 2.0 ** 80))
    def _():
        lax.fori_loop(0, tiles, again, 0)

    def finish(t, c):
        weight = acc[t, pl.ds(width, 1), :]
        some = weight > 0
        weight = jnp.where(some, weight, 1.0)
        o_ref[t] = (acc[t, :width, :] * (1.0 / weight)).T.astype(jnp.bfloat16)
        lse_ref[t] = jnp.where(some, top[t] + jnp.log2(weight), -1e30)
        return c

    lax.fori_loop(0, tiles, finish, 0, unroll=4)


def attend(half, q_pos, k_pos, q, kv):
    tiles, lanes, width = q.shape
    groups, _, each, piece, _ = kv.shape
    keys = groups * each * piece
    smem = pl.BlockSpec(memory_space=pltpu.SMEM)
    vmem = pl.BlockSpec(memory_space=pltpu.VMEM)
    return pl.pallas_call(
        attend_kernel,
        out_shape=(jax.ShapeDtypeStruct(q.shape, jnp.bfloat16),
                   jax.ShapeDtypeStruct((tiles, 1, lanes), jnp.float32)),
        in_specs=[smem, smem, smem, vmem, vmem],
        out_specs=(vmem, vmem),
        scratch_shapes=[
            pltpu.VMEM((CHUNK + keys, width), jnp.bfloat16),
            pltpu.VMEM((keys, width), jnp.bfloat16),
            pltpu.VMEM(((CHUNK + keys) // width, width + 16, width), jnp.bfloat16),
            pltpu.VMEM((tiles + 1, 2 * width, lanes), jnp.bfloat16),
            [pltpu.VMEM((CHUNK, lanes), jnp.bfloat16)] * 2,
            pltpu.VMEM((tiles + 1, width + 16, lanes), jnp.float32),
            pltpu.VMEM((tiles + 1, 1, lanes), jnp.float32),
        ],
        compiler_params=pltpu.CompilerParams(vmem_limit_bytes=26 * 1024 * 1024),
    )(half, q_pos, k_pos, q, kv)


def return_kernel(o_ref, lse_ref, o_all, lse_all, o_send, o_recv, l_send, l_recv, own_sem):
    x, z, c, y = place()
    steps, mates = row_mates(x, z, c, y)
    greet(mates)
    keep = [pltpu.make_async_copy(o_ref.at[x, c], o_all.at[x, c], own_sem.at[0]),
            pltpu.make_async_copy(lse_ref.at[x, c], lse_all.at[x, c], own_sem.at[1])]
    copies = []
    for n, (dx, dc) in enumerate(steps):
        to_x, to_c = (x + dx) % ROW, (c + dc) % 2
        for src, dst, send, recv in ((lse_ref, lse_all, l_send, l_recv), (o_ref, o_all, o_send, o_recv)):
            copy = pltpu.make_async_remote_copy(
                src_ref=src.at[to_x, to_c], dst_ref=dst.at[x, c], send_sem=send.at[n], recv_sem=recv.at[n],
                device_id=mates[n], device_id_type=MESH)
            copy.start()
            copies.append(copy)
    for copy in keep:
        copy.start()
    for copy in keep:
        copy.wait()
    for copy in copies:
        copy.wait()


def send_back(o, lse):
    sem = pltpu.SemaphoreType.DMA
    vmem = pl.BlockSpec(memory_space=pltpu.VMEM)
    n = 2 * ROW - 1
    return pl.pallas_call(
        return_kernel,
        out_shape=(jax.ShapeDtypeStruct(o.shape, o.dtype), jax.ShapeDtypeStruct(lse.shape, lse.dtype)),
        in_specs=[vmem, vmem],
        out_specs=(vmem, vmem),
        scratch_shapes=[sem((n,)), sem((n,)), sem((n,)), sem((n,)), sem((2,))],
        compiler_params=pltpu.CompilerParams(
            collective_id=1, has_side_effects=True, vmem_limit_bytes=32 * 1024 * 1024),
        cost_estimate=pl.CostEstimate(flops=0, bytes_accessed=20_000_000, transcendentals=0),
    )(o, lse)


def body(stored_query_rows, stored_key_rows, stored_value_rows, span_order):
    rows, heads, width = stored_query_rows.shape
    each = 2
    span = rows // each
    x, z, c, _ = place()
    q = stored_query_rows.reshape(each, span, 2, 2, 2, width).transpose(2, 3, 0, 4, 1, 5)
    q = q.reshape(2, 2, each, 2 * span, width)
    kv = jnp.stack([stored_key_rows, stored_value_rows])
    kv = kv.reshape(2, each, 2, span // 2, 2, width).transpose(4, 2, 0, 1, 3, 5)
    kv = kv.reshape(4, 2, each, span // 2, width)
    q_all, kv_all = gather(q, kv)

    order = span_order.reshape(RING // 2, 2, ROW, 2, each)
    k_pos = order.transpose(1, 0, 3, 2, 4).reshape(-1)
    in_row = lax.dynamic_index_in_dim(lax.dynamic_index_in_dim(order, z // 2, 0, False), z % 2, 2, False)
    q_pos = in_row.transpose(1, 0, 2).reshape(-1)
    half = jnp.reshape(x // 2, (1,)).astype(jnp.int32)
    o, lse = attend(half, q_pos, k_pos, q_all.reshape(2 * ROW * each, 2 * span, width),
                    kv_all.reshape(2 * RING * ROW, 2, each, span // 2, width))

    o, lse = send_back(o.reshape(ROW, 2, each, 2 * span, width), lse.reshape(ROW, 2, each, 1, 2 * span))
    o = o.reshape(2, 2, 2, each, 2, span, width)
    lse = lse.reshape(2, 2, 2, each, 2, span)
    top = jnp.max(lse, axis=0)
    weights = jnp.exp2(lse - top)
    share = weights / jnp.sum(weights, axis=0)
    result = jnp.sum(o.astype(jnp.float32) * share[..., None], axis=0).astype(jnp.bfloat16)
    return result.transpose(2, 4, 0, 1, 3, 5).reshape(rows, heads, width)


def solution(mesh):
    placed = (
        P(("outer", "inner"), "head", None),
        P(("outer", "inner"), "head", None),
        P(("outer", "inner"), "head", None),
        P(),
    )
    return jax.shard_map(
        body,
        mesh=mesh,
        in_specs=placed,
        out_specs=P(("outer", "inner"), "head", None),
        check_vma=False,
    )
```

```python
import math

import jax
import jax.numpy as jnp
from jax import lax
from jax.experimental import pallas as pl
from jax.experimental.pallas import tpu as pltpu
from jax.sharding import PartitionSpec as P

ROW = 4
RING = 8
EACH = 2
MESH = pl.DeviceIdType.MESH
NEVER = 2.0**20


def place():
    outer, inner = lax.axis_index("outer"), lax.axis_index("inner")
    return inner // 2, outer // 2 * 2 + inner % 2, outer % 2, lax.axis_index("head")


def device(x, z, c, y):
    return (z // 2 * 2 + c, x * 2 + z % 2, y)


def greet(peers):
    barrier = pltpu.get_barrier_semaphore()
    for peer in peers:
        pl.semaphore_signal(barrier, inc=1, device_id=peer, device_id_type=MESH)
    pl.semaphore_wait(barrier, len(peers))


def row_mates(x, z, c, y):
    steps = [(dx, dc) for dx in range(ROW) for dc in range(2) if (dx, dc) != (0, 0)]
    return steps, [device((x + dx) % ROW, z, (c + dc) % 2, y) for dx, dc in steps]


def remote(src, dst, send, recv, to):
    return pltpu.make_async_remote_copy(
        src_ref=src, dst_ref=dst, send_sem=send, recv_sem=recv, device_id=to, device_id_type=MESH)


def attend_kernel(place_ref, q_ref, kv_ref, q_all, kv_all, acc, top,
                  v_turned, q_turned, marks, p_bufs, relay,
                  q_send, q_recv, far_send, far_recv, on_send, on_recv, x_send, x_recv,
                  up_send, up_recv, down_send, down_recv, core_send, core_recv, own_sem):
    x, z, c, y = place()
    steps, mates = row_mates(x, z, c, y)
    mate = dict(zip(steps, mates))
    above, below = device(x, (z + 1) % RING, c, y), device(x, (z + RING - 1) % RING, c, y)
    partner = mate[0, 1]
    greet([*mates, above, below])
    piece, width = kv_ref.shape[-2:]
    block = 2 * piece
    lanes = q_ref.shape[-2]
    tiles = 2 * ROW * EACH
    window = 2 * ROW * EACH * piece
    rate = math.log2(math.e) / math.sqrt(width)
    half = x // 2
    role = x % 2 * 2 + x // 2
    mine = kv_ref.at[role]

    def slot_of(off, j):
        return kv_all.at[c, (z + off + RING) % RING, (x + j) % ROW]

    def pass_up(t, j, src):
        remote(src, slot_of(-t, j), up_send.at[t, j], up_recv.at[t, j], above).start()

    def pass_down(t, j, src):
        remote(src, slot_of(t, j), down_send.at[t, j], down_recv.at[t, j], below).start()

    def to_partner(off, j, src):
        r = (off + RING) % RING
        remote(src, slot_of(off, j), core_send.at[r, j], core_recv.at[r, j], partner).start()

    def arrived(dst, recv):
        remote(dst, dst, x_send.at[1], recv, partner).wait_recv()

    def gone(src, send):
        remote(src, src, send, x_recv.at[1], partner).wait_send()

    pass_up(0, 0, mine)
    pass_down(0, 0, mine)
    for d in (1, 3, 2):
        to = (x + d) % ROW
        remote(kv_ref.at[to % 2 * 2 + to // 2], kv_all.at[c, z, x], x_send.at[d], x_recv.at[d],
               device(to, z, c, y)).start()
    to_partner(0, 0, mine)
    keep_kv = pltpu.make_async_copy(mine, kv_all.at[c, z, x], own_sem.at[0])
    keep_q = pltpu.make_async_copy(q_ref.at[x % 2, c], q_all.at[x, c], own_sem.at[1])
    keep_kv.start()
    keep_q.start()
    for side, dx in ((0, 1), (1, 3)):
        for dc in range(2):
            remote(q_ref.at[x % 2, (c + dc) % 2, side], relay.at[side, dc], far_send.at[side, dc],
                   far_recv.at[side, dc], mate[dx, 0]).start()
    for n, (dx, dc) in enumerate(steps):
        if dx != 2:
            remote(q_ref.at[(x + dx) % 2, (c + dc) % 2], q_all.at[x, c], q_send.at[n], q_recv.at[n],
                   mates[n]).start()

    k_row = lax.broadcasted_iota(jnp.int32, (window, width), 0)
    column = lax.broadcasted_iota(jnp.int32, (window, width), 1)
    marks[...] = jnp.where((column == k_row // piece) | (column == tiles), 1.0, 0.0).astype(marks.dtype)
    q_turned[:, width + tiles:, :] = jnp.zeros((tiles, width - tiles, lanes), q_turned.dtype)
    v_turned[:, width:, :] = jnp.ones((v_turned.shape[0], v_turned.shape[1] - width, width), v_turned.dtype)

    for j in (1, 3, 2):
        slot = slot_of(0, j)
        arrived(slot, x_recv.at[ROW - j])
        pass_up(0, j, slot)
        pass_down(0, j, slot)
        to_partner(0, j, slot)
    for side, dx in ((0, 1), (1, 3)):
        for dc in range(2):
            arrived(relay.at[side, dc], far_recv.at[side, dc])
            remote(relay.at[side, dc], q_all.at[(x + ROW - dx) % ROW, c, side], on_send.at[side, dc],
                   on_recv.at[side, dc], mate[dx, dc]).start()
    keep_kv.wait()
    keep_q.wait()

    def ready(zc):
        r = (zc - z + RING) % RING
        for j in range(ROW):
            arrived(kv_all.at[1 - c, zc, (x + j) % ROW], core_recv.at[r, j])
        for core in range(2):
            for at in range(ROW):
                v = kv_all[core, zc, at, 1].reshape(EACH * piece, width)
                v_turned[(core * RING + zc) * ROW + at, :width, :] = v.T

    ready(z)

    own_k = lax.broadcasted_iota(jnp.int32, (piece, lanes), 0) + half * piece
    own_allowed = own_k <= lax.broadcasted_iota(jnp.int32, (piece, lanes), 1) % block

    def take(at, core):
        for b in range(EACH):
            t = (at * 2 + core) * EACH + b
            q = q_all[at, core, b].T
            q_turned[t, :width, :] = q
            s = jnp.dot(kv_all[core, z, at, 0, b], q, preferred_element_type=jnp.float32)
            ref = jnp.max(s, axis=0, keepdims=True).astype(jnp.bfloat16).astype(jnp.float32)
            top[t] = ref
            first = lax.broadcasted_iota(jnp.int32, (tiles, lanes), 0) == 0
            q_turned[t, width + tiles:width + 2 * tiles, :] = jnp.where(first, -ref, 0.0).astype(q_turned.dtype)
            p = jnp.where(own_allowed, jnp.exp2((s - ref) * rate), 0.0).astype(jnp.bfloat16)
            v = v_turned[(core * RING + z) * ROW + at]
            acc[t] = jnp.dot(v[:, b * piece:(b + 1) * piece], p, preferred_element_type=jnp.float32)

    take(x, c)
    arrived(q_all.at[x, 1 - c], q_recv.at[steps.index((0, 1))])
    take(x, 1 - c)
    for dx in (1, 3):
        for dc in range(2):
            core = (c + dc) % 2
            arrived(q_all.at[(x + ROW - dx) % ROW, core], q_recv.at[steps.index((dx, dc))])
            take((x + ROW - dx) % ROW, core)
    for dc in range(2):
        core = (c + dc) % 2
        for side in range(2):
            arrived(q_all.at[(x + 2) % ROW, core, side], on_recv.at[side, dc])
        take((x + 2) % ROW, core)

    def row_at(n):
        off = jnp.where(n % 2 == 1, -((n + 1) // 2), n // 2)
        return off, (z + off + RING) % RING

    def weigh(t, zc, buf):
        own = (t // EACH % 2 * ROW + t // (2 * EACH)) * EACH + t % EACH
        before = place_ref[zc] < place_ref[z, pl.ds(own, 1), :]
        q_turned[t, width:width + tiles, :] = jnp.where(before, 0.0, -NEVER).astype(q_turned.dtype)
        k = [kv_all[core, zc, at, 0].reshape(EACH * piece, width) for core in range(2) for at in range(ROW)]
        keys = jnp.concatenate([jnp.concatenate(k, axis=0), marks[...]], axis=1)
        s = jnp.dot(keys, q_turned[t], preferred_element_type=jnp.float32)
        p_bufs[buf][...] = jnp.exp2(s * rate).astype(jnp.bfloat16)

    def absorb(t, zc, buf):
        v = [v_turned[(core * RING + zc) * ROW + at] for core in range(2) for at in range(ROW)]
        acc[t] += jnp.dot(jnp.concatenate(v, axis=1), p_bufs[buf][...], preferred_element_type=jnp.float32)

    def relay_on(n, j):
        t = n // 2 + 1
        rising = n % 2 == 0

        @pl.when((n < 6) & rising)
        def _():
            slot = slot_of(-t, j)
            arrived(slot, up_recv.at[t - 1, j])

            @pl.when((t < 3) | (j < 2))
            def _():
                pass_up(t, j, slot)

            to_partner(-t, j, slot)

        @pl.when((n < 6) & jnp.logical_not(rising))
        def _():
            slot = slot_of(t, j)
            arrived(slot, down_recv.at[t - 1, j])

            @pl.when((t < 3) | (j >= 2))
            def _():
                pass_down(t, j, slot)

            to_partner(t, j, slot)

        @pl.when(n == 6)
        def _():
            slot = slot_of(RING // 2, j)
            arrived(slot, up_recv.at[3, j] if j < 2 else down_recv.at[3, j])
            to_partner(RING // 2, j, slot)

    per_turn = 4
    turns = tiles // per_turn

    def turn(m, carry):
        n, i = m // turns, m % turns
        _, zc = row_at(n)
        _, ahead = row_at(jnp.minimum(n + 1, RING - 1))

        @pl.when(i == 0)
        def _():
            relay_on(n, 0)
            relay_on(n, 1)

        @pl.when(i == 1)
        def _():
            relay_on(n, 3)

        @pl.when(i == 2)
        def _():
            relay_on(n, 2)

        @pl.when((i == turns - 1) & (n < RING - 1))
        def _():
            ready(ahead)

        for u in range(per_turn):
            t = i * per_turn + u
            wrap = t == tiles - 1
            weigh(jnp.where(wrap, 0, t + 1), jnp.where(wrap, ahead, zc), 1 - u % 2)
            absorb(t, zc, u % 2)
        return carry

    weigh(0, z, 0)
    lax.fori_loop(0, RING * turns, turn, 0)

    for j in range(ROW):
        for t in range(RING // 2):
            if t < 3 or j < 2:
                gone(slot_of(0, j), up_send.at[t, j])
            if t < 3 or j >= 2:
                gone(slot_of(0, j), down_send.at[t, j])
        for r in range(RING):
            gone(slot_of(0, j), core_send.at[r, j])
        if j:
            gone(slot_of(0, j), x_send.at[j])
    for side in range(2):
        for dc in range(2):
            gone(relay.at[side, dc], far_send.at[side, dc])
            gone(relay.at[side, dc], on_send.at[side, dc])
    for n, (dx, dc) in enumerate(steps):
        if dx != 2:
            gone(q_all.at[x, c], q_send.at[n])


def attend(places, q, kv):
    sem = pltpu.SemaphoreType.DMA
    half_ring = RING // 2
    vmem = pl.BlockSpec(memory_space=pltpu.VMEM)
    lanes, width = q.shape[-2:]
    piece = kv.shape[-2]
    tiles = 2 * ROW * EACH
    window = tiles * piece
    return pl.pallas_call(
        attend_kernel,
        out_shape=(jax.ShapeDtypeStruct((ROW, 2, *q.shape[2:]), q.dtype),
                   jax.ShapeDtypeStruct((2, RING, ROW, *kv.shape[1:]), kv.dtype),
                   jax.ShapeDtypeStruct((tiles, width + 16, lanes), jnp.float32),
                   jax.ShapeDtypeStruct((tiles, 1, lanes), jnp.float32)),
        in_specs=[vmem] * 3,
        out_specs=(vmem,) * 4,
        scratch_shapes=[
            pltpu.VMEM((2 * RING * ROW, width + 16, width), jnp.bfloat16),
            pltpu.VMEM((tiles, 2 * width, lanes), jnp.bfloat16),
            pltpu.VMEM((window, width), jnp.bfloat16),
            [pltpu.VMEM((window, lanes), jnp.bfloat16)] * 2,
            pltpu.VMEM((2, 2, lanes, width), jnp.bfloat16),
            sem((2 * ROW - 1,)), sem((2 * ROW - 1,)), sem((2, 2)), sem((2, 2)), sem((2, 2)), sem((2, 2)),
            sem((ROW,)), sem((ROW,)),
            sem((half_ring, ROW)), sem((half_ring, ROW)), sem((half_ring, ROW)), sem((half_ring, ROW)),
            sem((RING, ROW)), sem((RING, ROW)), sem((2,)),
        ],
        compiler_params=pltpu.CompilerParams(
            collective_id=0, has_side_effects=True, vmem_limit_bytes=32 * 1024 * 1024),
        cost_estimate=pl.CostEstimate(flops=10**10, bytes_accessed=20_000_000, transcendentals=0),
    )(places, q, kv)


def finish_kernel(place_ref, order, q_all, kv_all, acc, top, o_ref, lse_ref, again_acc, again_top):
    x, z, _, _ = place()
    half = x // 2
    tiles, deep, lanes = acc.shape
    piece, width = kv_all.shape[-2:]
    block = 2 * piece
    rate = math.log2(math.e) / math.sqrt(width)
    q_row = lax.broadcasted_iota(jnp.int32, (1, lanes), 1) % block

    def stored(zc, core, at, b):
        return order[((zc // 2 * 2 + core) * RING + at * 2 + zc % 2) * EACH + b]

    def put(t, weight, sums, reference):
        some = weight > 0
        weight = jnp.where(some, weight, 1.0)
        o_ref[t] = (sums * (1.0 / weight)).T.astype(jnp.bfloat16)
        lse_ref[t] = jnp.where(some, reference + jnp.log2(weight), -1e30)

    worst = jnp.zeros((1, lanes), jnp.float32)
    for t in range(tiles):
        weight = acc[t, width:width + 1, :]
        own = (t // EACH % 2 * ROW + t // (2 * EACH)) * EACH + t % EACH
        no_key = (place_ref[z, own:own + 1, :] == 0) & (q_row < half * piece)
        fits = ((weight > 2.0**-60) & (weight < 2.0**80)) | no_key
        worst = jnp.maximum(worst, jnp.where(fits, 0.0, 1.0))
        put(t, weight, acc[t, :width, :], top[t] * rate)

    def redo(t, carry):
        at_q, core_q, b_q = t // (2 * EACH), t // EACH % 2, t % EACH
        pos = stored(z, core_q, at_q, b_q)
        q = q_all[at_q, core_q, b_q].T
        again_acc[...] = jnp.zeros_like(again_acc)
        again_top[0:1, :] = jnp.full((1, lanes), -1e30, jnp.float32)
        again_top[1:2, :] = jnp.zeros((1, lanes), jnp.float32)

        def one(g, carry):
            core, zc, at = g // (RING * ROW), g // ROW % RING, g % ROW
            for b in range(EACH):
                kp = stored(zc, core, at, b)
                k_at = lax.broadcasted_iota(jnp.int32, (piece, lanes), 0) + half * piece + kp * block
                s = jnp.dot(kv_all[core, zc, at, 0, b], q, preferred_element_type=jnp.float32) * rate
                s = jnp.where(k_at <= pos * block + q_row, s, -2e30)
                old = again_top[0:1, :]
                new = jnp.maximum(old, jnp.max(s, axis=0, keepdims=True))
                p = jnp.exp2(s - new)
                fade = jnp.exp2(old - new)
                again_top[0:1, :] = new
                again_top[1:2, :] = again_top[1:2, :] * fade + jnp.sum(p, axis=0, keepdims=True)
                v = kv_all[core, zc, at, 1, b].T
                again_acc[...] = again_acc[...] * fade + jnp.dot(
                    v, p.astype(jnp.bfloat16), preferred_element_type=jnp.float32)
            return carry

        lax.fori_loop(0, 2 * RING * ROW, one, 0)
        put(t, again_top[1:2, :], again_acc[...], again_top[0:1, :])
        return carry

    @pl.when(jnp.max(worst) > 0)
    def _():
        lax.fori_loop(0, tiles, redo, 0)


def finish(places, order, q_all, kv_all, acc, top):
    smem = pl.BlockSpec(memory_space=pltpu.SMEM)
    vmem = pl.BlockSpec(memory_space=pltpu.VMEM)
    tiles, deep, lanes = acc.shape
    width = deep - 16
    return pl.pallas_call(
        finish_kernel,
        out_shape=(jax.ShapeDtypeStruct((tiles, lanes, width), jnp.bfloat16),
                   jax.ShapeDtypeStruct((tiles, 1, lanes), jnp.float32)),
        in_specs=[vmem, smem, vmem, vmem, vmem, vmem],
        out_specs=(vmem, vmem),
        scratch_shapes=[pltpu.VMEM((width, lanes), jnp.float32), pltpu.VMEM((8, lanes), jnp.float32)],
        compiler_params=pltpu.CompilerParams(vmem_limit_bytes=20 * 1024 * 1024),
    )(places, order, q_all, kv_all, acc, top)


def return_kernel(o_ref, lse_ref, o_all, lse_all, relay, o_send, o_recv, l_send, l_recv,
                  far_send, far_recv, on_send, on_recv, own_sem):
    x, z, c, y = place()
    steps, mates = row_mates(x, z, c, y)
    mate = dict(zip(steps, mates))
    greet(mates)
    keep = [pltpu.make_async_copy(o_ref.at[x, c], o_all.at[x, c], own_sem.at[0]),
            pltpu.make_async_copy(lse_ref.at[x, c], lse_all.at[x, c], own_sem.at[1])]
    copies, far = [], []
    for side, dx in ((0, 1), (1, 3)):
        for dc in range(2):
            far.append(remote(o_ref.at[(x + 2) % ROW, (c + dc) % 2, side], relay.at[side, dc],
                              far_send.at[side, dc], far_recv.at[side, dc], mate[dx, 0]))
            far[-1].start()
    for n, (dx, dc) in enumerate(steps):
        to_x, to_c = (x + dx) % ROW, (c + dc) % 2
        copies.append(remote(lse_ref.at[to_x, to_c], lse_all.at[x, c], l_send.at[n], l_recv.at[n], mates[n]))
        copies[-1].start()
        if dx != 2:
            copies.append(remote(o_ref.at[to_x, to_c], o_all.at[x, c], o_send.at[n], o_recv.at[n], mates[n]))
            copies[-1].start()
    for copy in keep:
        copy.start()
    for k, (side, dx) in enumerate(((0, 1), (1, 3))):
        for dc in range(2):
            far[2 * k + dc].wait()
            copies.append(remote(relay.at[side, dc], o_all.at[(x + ROW - dx) % ROW, c, side],
                                 on_send.at[side, dc], on_recv.at[side, dc], mate[dx, dc]))
            copies[-1].start()
    for copy in [*keep, *copies]:
        copy.wait()


def send_back(o, lse):
    sem = pltpu.SemaphoreType.DMA
    vmem = pl.BlockSpec(memory_space=pltpu.VMEM)
    n = 2 * ROW - 1
    return pl.pallas_call(
        return_kernel,
        out_shape=(jax.ShapeDtypeStruct(o.shape, o.dtype), jax.ShapeDtypeStruct(lse.shape, lse.dtype)),
        in_specs=[vmem, vmem],
        out_specs=(vmem, vmem),
        scratch_shapes=[pltpu.VMEM((2, 2, *o.shape[-2:]), o.dtype),
                        sem((n,)), sem((n,)), sem((n,)), sem((n,)),
                        sem((2, 2)), sem((2, 2)), sem((2, 2)), sem((2, 2)), sem((2,))],
        compiler_params=pltpu.CompilerParams(
            collective_id=1, has_side_effects=True, vmem_limit_bytes=32 * 1024 * 1024),
        cost_estimate=pl.CostEstimate(flops=0, bytes_accessed=20_000_000, transcendentals=0),
    )(o, lse)


def body(stored_query_rows, stored_key_rows, stored_value_rows, span_order):
    rows, heads, width = stored_query_rows.shape
    span = rows // EACH
    q = stored_query_rows.reshape(EACH, span, 2, 2, 2, width).transpose(2, 3, 0, 4, 1, 5)
    q = q.reshape(2, 2, EACH, 2 * span, width)
    kv = jnp.stack([stored_key_rows, stored_value_rows])
    kv = kv.reshape(2, EACH, 2, span // 2, 2, width).transpose(4, 2, 0, 1, 3, 5)
    kv = kv.reshape(4, 2, EACH, span // 2, width)
    places = span_order.astype(jnp.float32).reshape(RING // 2, 2, ROW, 2, EACH).transpose(0, 3, 1, 2, 4)
    places = jnp.broadcast_to(places.reshape(RING, 2 * ROW * EACH, 1), (RING, 2 * ROW * EACH, 2 * span))
    o, lse = finish(places, span_order, *attend(places, q, kv))

    o, lse = send_back(o.reshape(ROW, 2, EACH, 2 * span, width), lse.reshape(ROW, 2, EACH, 1, 2 * span))
    o = o.reshape(2, 2, 2, EACH, 2, span, width)
    lse = lse.reshape(2, 2, 2, EACH, 2, span)
    top = jnp.max(lse, axis=0)
    weights = jnp.exp2(lse - top)
    share = weights / jnp.sum(weights, axis=0)
    result = jnp.sum(o.astype(jnp.float32) * share[..., None], axis=0).astype(jnp.bfloat16)
    return result.transpose(2, 4, 0, 1, 3, 5).reshape(rows, heads, width)


def solution(mesh):
    placed = (
        P(("outer", "inner"), "head", None),
        P(("outer", "inner"), "head", None),
        P(("outer", "inner"), "head", None),
        P(),
    )
    return jax.shard_map(
        body,
        mesh=mesh,
        in_specs=placed,
        out_specs=P(("outer", "inner"), "head", None),
        check_vma=False,
    )
```

```python
import math

import jax
import jax.numpy as jnp
from jax import lax
from jax.experimental import pallas as pl
from jax.experimental.pallas import tpu as pltpu
from jax.sharding import PartitionSpec as P

ROW = 4
RING = 8
EACH = 2
MESH = pl.DeviceIdType.MESH
NEVER = 2.0**20


def place():
    outer, inner = lax.axis_index("outer"), lax.axis_index("inner")
    return inner // 2, outer // 2 * 2 + inner % 2, outer % 2, lax.axis_index("head")


def device(x, z, c, y):
    return (z // 2 * 2 + c, x * 2 + z % 2, y)


def greet(peers):
    barrier = pltpu.get_barrier_semaphore()
    for peer in peers:
        pl.semaphore_signal(barrier, inc=1, device_id=peer, device_id_type=MESH)
    pl.semaphore_wait(barrier, len(peers))


def row_mates(x, z, c, y):
    steps = [(dx, dc) for dx in range(ROW) for dc in range(2) if (dx, dc) != (0, 0)]
    return steps, [device((x + dx) % ROW, z, (c + dc) % 2, y) for dx, dc in steps]


def remote(src, dst, send, recv, to):
    return pltpu.make_async_remote_copy(
        src_ref=src, dst_ref=dst, send_sem=send, recv_sem=recv, device_id=to, device_id_type=MESH)


def attend_kernel(place_ref, q_ref, kv_ref, q_all, kv_all, acc, total, top,
                  v_turned, q_turned, marks, p_bufs, relay,
                  q_send, q_recv, far_send, far_recv, on_send, on_recv, x_send, x_recv,
                  up_send, up_recv, down_send, down_recv, core_send, core_recv, own_sem):
    x, z, c, y = place()
    steps, mates = row_mates(x, z, c, y)
    mate = dict(zip(steps, mates))
    above, below = device(x, (z + 1) % RING, c, y), device(x, (z + RING - 1) % RING, c, y)
    partner = mate[0, 1]
    greet([*mates, above, below])
    piece, width = kv_ref.shape[-2:]
    block = 2 * piece
    lanes = q_ref.shape[-2]
    tiles = 2 * ROW * EACH
    window = 2 * ROW * EACH * piece
    rate = math.log2(math.e) / math.sqrt(width)
    half = x // 2
    role = x % 2 * 2 + x // 2
    mine = kv_ref.at[role]

    def slot_of(off, j):
        return kv_all.at[c, (z + off + RING) % RING, (x + j) % ROW]

    def pass_up(t, j, src):
        remote(src, slot_of(-t, j), up_send.at[t, j], up_recv.at[t, j], above).start()

    def pass_down(t, j, src):
        remote(src, slot_of(t, j), down_send.at[t, j], down_recv.at[t, j], below).start()

    def to_partner(off, j, src):
        r = (off + RING) % RING
        remote(src, slot_of(off, j), core_send.at[r, j], core_recv.at[r, j], partner).start()

    def arrived(dst, recv):
        remote(dst, dst, x_send.at[1], recv, partner).wait_recv()

    def gone(src, send):
        remote(src, src, send, x_recv.at[1], partner).wait_send()

    pass_up(0, 0, mine)
    pass_down(0, 0, mine)
    for d in (1, 3, 2):
        to = (x + d) % ROW
        remote(kv_ref.at[to % 2 * 2 + to // 2], kv_all.at[c, z, x], x_send.at[d], x_recv.at[d],
               device(to, z, c, y)).start()
    to_partner(0, 0, mine)
    keep_kv = pltpu.make_async_copy(mine, kv_all.at[c, z, x], own_sem.at[0])
    keep_q = pltpu.make_async_copy(q_ref.at[x % 2, c], q_all.at[x, c], own_sem.at[1])
    keep_kv.start()
    keep_q.start()
    for n, (dx, dc) in enumerate(steps):
        if dx != 2:
            remote(q_ref.at[(x + dx) % 2, (c + dc) % 2], q_all.at[x, c], q_send.at[n], q_recv.at[n],
                   mates[n]).start()
    for side, dx in ((0, 1), (1, 3)):
        for dc in range(2):
            remote(q_ref.at[x % 2, (c + dc) % 2, side], relay.at[side, dc], far_send.at[side, dc],
                   far_recv.at[side, dc], mate[dx, 0]).start()

    k_row = lax.broadcasted_iota(jnp.int32, (window, width), 0)
    column = lax.broadcasted_iota(jnp.int32, (window, width), 1)
    marks[...] = jnp.where((column == k_row // piece) | (column == tiles), 1.0, 0.0).astype(marks.dtype)
    q_turned[:, width + tiles:, :] = jnp.zeros((tiles, width - tiles, lanes), q_turned.dtype)

    for j in (1, 3, 2):
        slot = slot_of(0, j)
        arrived(slot, x_recv.at[ROW - j])
        pass_up(0, j, slot)
        pass_down(0, j, slot)
        to_partner(0, j, slot)
    keep_kv.wait()
    keep_q.wait()

    def forward():
        for side, dx in ((0, 1), (1, 3)):
            for dc in range(2):
                arrived(relay.at[side, dc], far_recv.at[side, dc])
                remote(relay.at[side, dc], q_all.at[(x + ROW - dx) % ROW, c, side], on_send.at[side, dc],
                       on_recv.at[side, dc], mate[dx, dc]).start()

    def ready(zc):
        r = (zc - z + RING) % RING
        for j in range(ROW):
            arrived(kv_all.at[1 - c, zc, (x + j) % ROW], core_recv.at[r, j])
        for core in range(2):
            for at in range(ROW):
                v = kv_all[core, zc, at, 1].reshape(EACH * piece, width)
                v_turned[(core * RING + zc) * ROW + at] = v.T

    ready(z)

    own_k = lax.broadcasted_iota(jnp.int32, (piece, lanes), 0) + half * piece
    own_allowed = own_k <= lax.broadcasted_iota(jnp.int32, (piece, lanes), 1) % block

    def take(at, core):
        for b in range(EACH):
            t = (at * 2 + core) * EACH + b
            q = q_all[at, core, b].T
            q_turned[t, :width, :] = q
            s = jnp.dot(kv_all[core, z, at, 0, b], q, preferred_element_type=jnp.float32)
            ref = jnp.max(s, axis=0, keepdims=True).astype(jnp.bfloat16).astype(jnp.float32)
            top[t] = ref
            first = lax.broadcasted_iota(jnp.int32, (tiles, lanes), 0) == 0
            q_turned[t, width + tiles:width + 2 * tiles, :] = jnp.where(first, -ref, 0.0).astype(q_turned.dtype)
            p = jnp.where(own_allowed, jnp.exp2((s - ref) * rate), 0.0)
            total[t] = jnp.sum(p.reshape(piece // 8, 8, lanes), axis=0)
            v = v_turned[(core * RING + z) * ROW + at]
            acc[t] = jnp.dot(v[:, b * piece:(b + 1) * piece], p.astype(jnp.bfloat16), preferred_element_type=jnp.float32)

    take(x, c)
    arrived(q_all.at[x, 1 - c], q_recv.at[steps.index((0, 1))])
    take(x, 1 - c)

    def await_queries(dx):
        for core in range(2):
            if dx == 2:
                for side in range(2):
                    dc = (core + c) % 2
                    arrived(q_all.at[(x + 2) % ROW, core, side], on_recv.at[side, dc])
            else:
                dc = (core + c) % 2
                arrived(q_all.at[(x + ROW - dx) % ROW, core], q_recv.at[steps.index((dx, 0)) + dc])

    def row_at(n):
        off = jnp.where(n % 2 == 1, -((n + 1) // 2), n // 2)
        return off, (z + off + RING) % RING

    def weigh(t, zc, buf):
        own = (t // EACH % 2 * ROW + t // (2 * EACH)) * EACH + t % EACH
        before = place_ref[zc] < place_ref[z, pl.ds(own, 1), :]
        q_turned[t, width:width + tiles, :] = jnp.where(before, 0.0, -NEVER).astype(q_turned.dtype)
        k = [kv_all[core, zc, at, 0].reshape(EACH * piece, width) for core in range(2) for at in range(ROW)]
        keys = jnp.concatenate([jnp.concatenate(k, axis=0), marks[...]], axis=1)
        s = jnp.dot(keys, q_turned[t], preferred_element_type=jnp.float32)
        p = jnp.exp2(s * rate)
        total[t] += jnp.sum(p.reshape(window // 8, 8, lanes), axis=0)
        p_bufs[buf][...] = p.astype(jnp.bfloat16)

    def absorb(t, zc, buf):
        v = [v_turned[(core * RING + zc) * ROW + at] for core in range(2) for at in range(ROW)]
        acc[t] += jnp.dot(jnp.concatenate(v, axis=1), p_bufs[buf][...], preferred_element_type=jnp.float32)

    def relay_on(n, j):
        t = n // 2 + 1
        rising = n % 2 == 0

        @pl.when((n < 6) & rising)
        def _():
            slot = slot_of(-t, j)
            arrived(slot, up_recv.at[t - 1, j])

            @pl.when((t < 3) | (j < 2))
            def _():
                pass_up(t, j, slot)

            to_partner(-t, j, slot)

        @pl.when((n < 6) & jnp.logical_not(rising))
        def _():
            slot = slot_of(t, j)
            arrived(slot, down_recv.at[t - 1, j])

            @pl.when((t < 3) | (j >= 2))
            def _():
                pass_down(t, j, slot)

            to_partner(t, j, slot)

        @pl.when(n == 6)
        def _():
            slot = slot_of(RING // 2, j)
            arrived(slot, up_recv.at[3, j] if j < 2 else down_recv.at[3, j])
            to_partner(RING // 2, j, slot)

    for j in (0, 1, 3, 2):
        relay_on(0, j)
        relay_on(1, j)

    per_turn = 2 * EACH
    turns = ROW * RING
    early = 3

    def plan(m):
        first = m < early * ROW
        n = jnp.where(first, m % early, m // ROW)
        g = jnp.where(first, m // early, m % ROW)
        chip = (x + jnp.where(g == 1, 3, jnp.where(g == 2, 1, jnp.where(g == 3, 2, 0)))) % ROW
        return chip, chip * per_turn, row_at(n)[1]

    def turn(m, carry):
        _, base, zc = plan(m)
        chip, next_base, next_zc = plan(m + 1)
        n, i = m // ROW, m % ROW

        @pl.when((m < early - 1) | ((m >= 2 * ROW) & (i == ROW - 1) & (m < turns - 1)))
        def _():
            ready(next_zc)

        for g, dx in ((1, 1), (2, 3), (3, 2)):
            @pl.when(m == early * g - 1)
            def _(dx=dx):
                await_queries(dx)

        @pl.when(m == early + 1)
        def _():
            forward()

        @pl.when((m == early - 1) | (m == 2 * early - 1) | (m == 3 * early - 1))
        def _():
            take(chip, 0)
            take(chip, 1)

        @pl.when((m >= 2 * ROW) & (i == 0))
        def _():
            relay_on(n, 0)
            relay_on(n, 1)

        @pl.when((m >= 2 * ROW) & (i == 1))
        def _():
            relay_on(n, 3)

        @pl.when((m >= 2 * ROW) & (i == 2))
        def _():
            relay_on(n, 2)

        for u in range(per_turn):
            done = u == per_turn - 1
            weigh(next_base if done else base + u + 1, next_zc if done else zc, 1 - u % 2)
            absorb(base + u, zc, u % 2)
        return carry

    weigh(x * per_turn, z, 0)
    lax.fori_loop(0, turns - 1, turn, 0)
    _, last_base, last_zc = plan(turns - 1)
    for u in range(per_turn):
        if u < per_turn - 1:
            weigh(last_base + u + 1, last_zc, 1 - u % 2)
        absorb(last_base + u, last_zc, u % 2)

    for j in range(ROW):
        for t in range(RING // 2):
            if t < 3 or j < 2:
                gone(slot_of(0, j), up_send.at[t, j])
            if t < 3 or j >= 2:
                gone(slot_of(0, j), down_send.at[t, j])
        for r in range(RING):
            gone(slot_of(0, j), core_send.at[r, j])
        if j:
            gone(slot_of(0, j), x_send.at[j])
    for side in range(2):
        for dc in range(2):
            gone(relay.at[side, dc], far_send.at[side, dc])
            gone(relay.at[side, dc], on_send.at[side, dc])
    for n, (dx, dc) in enumerate(steps):
        if dx != 2:
            gone(q_all.at[x, c], q_send.at[n])


def attend(places, q, kv):
    sem = pltpu.SemaphoreType.DMA
    half_ring = RING // 2
    vmem = pl.BlockSpec(memory_space=pltpu.VMEM)
    lanes, width = q.shape[-2:]
    piece = kv.shape[-2]
    tiles = 2 * ROW * EACH
    window = tiles * piece
    return pl.pallas_call(
        attend_kernel,
        out_shape=(jax.ShapeDtypeStruct((ROW, 2, *q.shape[2:]), q.dtype),
                   jax.ShapeDtypeStruct((2, RING, ROW, *kv.shape[1:]), kv.dtype),
                   jax.ShapeDtypeStruct((tiles, width, lanes), jnp.float32),
                   jax.ShapeDtypeStruct((tiles, 8, lanes), jnp.float32),
                   jax.ShapeDtypeStruct((tiles, 1, lanes), jnp.float32)),
        in_specs=[vmem] * 3,
        out_specs=(vmem,) * 5,
        scratch_shapes=[
            pltpu.VMEM((2 * RING * ROW, width, width), jnp.bfloat16),
            pltpu.VMEM((tiles, 2 * width, lanes), jnp.bfloat16),
            pltpu.VMEM((window, width), jnp.bfloat16),
            [pltpu.VMEM((window, lanes), jnp.bfloat16)] * 2,
            pltpu.VMEM((2, 2, lanes, width), jnp.bfloat16),
            sem((2 * ROW - 1,)), sem((2 * ROW - 1,)), sem((2, 2)), sem((2, 2)), sem((2, 2)), sem((2, 2)),
            sem((ROW,)), sem((ROW,)),
            sem((half_ring, ROW)), sem((half_ring, ROW)), sem((half_ring, ROW)), sem((half_ring, ROW)),
            sem((RING, ROW)), sem((RING, ROW)), sem((2,)),
        ],
        compiler_params=pltpu.CompilerParams(
            collective_id=0, has_side_effects=True, vmem_limit_bytes=32 * 1024 * 1024),
        cost_estimate=pl.CostEstimate(flops=10**10, bytes_accessed=20_000_000, transcendentals=0),
    )(places, q, kv)


def finish_kernel(place_ref, order, q_all, kv_all, acc, total, top, o_ref, lse_ref, again_acc, again_top):
    x, z, _, _ = place()
    half = x // 2
    tiles, _, lanes = acc.shape
    piece, width = kv_all.shape[-2:]
    block = 2 * piece
    rate = math.log2(math.e) / math.sqrt(width)
    q_row = lax.broadcasted_iota(jnp.int32, (1, lanes), 1) % block

    def stored(zc, core, at, b):
        return order[((zc // 2 * 2 + core) * RING + at * 2 + zc % 2) * EACH + b]

    def put(t, weight, sums, reference):
        some = weight > 0
        weight = jnp.where(some, weight, 1.0)
        o_ref[t] = (sums * (1.0 / weight)).T.astype(jnp.bfloat16)
        lse_ref[t] = jnp.where(some, reference + jnp.log2(weight), -1e30)

    worst = jnp.zeros((1, lanes), jnp.float32)
    for t in range(tiles):
        weight = jnp.sum(total[t], axis=0, keepdims=True)
        own = (t // EACH % 2 * ROW + t // (2 * EACH)) * EACH + t % EACH
        no_key = (place_ref[z, own:own + 1, :] == 0) & (q_row < half * piece)
        fits = ((weight > 2.0**-60) & (weight < 2.0**80)) | no_key
        worst = jnp.maximum(worst, jnp.where(fits, 0.0, 1.0))
        put(t, weight, acc[t], top[t] * rate)

    def redo(t, carry):
        at_q, core_q, b_q = t // (2 * EACH), t // EACH % 2, t % EACH
        pos = stored(z, core_q, at_q, b_q)
        q = q_all[at_q, core_q, b_q].T
        again_acc[...] = jnp.zeros_like(again_acc)
        again_top[0:1, :] = jnp.full((1, lanes), -1e30, jnp.float32)
        again_top[1:2, :] = jnp.zeros((1, lanes), jnp.float32)

        def one(g, carry):
            core, zc, at = g // (RING * ROW), g // ROW % RING, g % ROW
            for b in range(EACH):
                kp = stored(zc, core, at, b)
                k_at = lax.broadcasted_iota(jnp.int32, (piece, lanes), 0) + half * piece + kp * block
                s = jnp.dot(kv_all[core, zc, at, 0, b], q, preferred_element_type=jnp.float32) * rate
                s = jnp.where(k_at <= pos * block + q_row, s, -2e30)
                old = again_top[0:1, :]
                new = jnp.maximum(old, jnp.max(s, axis=0, keepdims=True))
                p = jnp.exp2(s - new)
                fade = jnp.exp2(old - new)
                again_top[0:1, :] = new
                again_top[1:2, :] = again_top[1:2, :] * fade + jnp.sum(p, axis=0, keepdims=True)
                v = kv_all[core, zc, at, 1, b].T
                again_acc[...] = again_acc[...] * fade + jnp.dot(
                    v, p.astype(jnp.bfloat16), preferred_element_type=jnp.float32)
            return carry

        lax.fori_loop(0, 2 * RING * ROW, one, 0)
        put(t, again_top[1:2, :], again_acc[...], again_top[0:1, :])
        return carry

    @pl.when(jnp.max(worst) > 0)
    def _():
        lax.fori_loop(0, tiles, redo, 0)


def finish(places, order, q_all, kv_all, acc, total, top):
    smem = pl.BlockSpec(memory_space=pltpu.SMEM)
    vmem = pl.BlockSpec(memory_space=pltpu.VMEM)
    tiles, width, lanes = acc.shape
    return pl.pallas_call(
        finish_kernel,
        out_shape=(jax.ShapeDtypeStruct((tiles, lanes, width), jnp.bfloat16),
                   jax.ShapeDtypeStruct((tiles, 1, lanes), jnp.float32)),
        in_specs=[vmem, smem, vmem, vmem, vmem, vmem, vmem],
        out_specs=(vmem, vmem),
        scratch_shapes=[pltpu.VMEM((width, lanes), jnp.float32), pltpu.VMEM((8, lanes), jnp.float32)],
        compiler_params=pltpu.CompilerParams(vmem_limit_bytes=20 * 1024 * 1024),
    )(places, order, q_all, kv_all, acc, total, top)


def return_kernel(o_ref, lse_ref, o_all, lse_all, relay, o_send, o_recv, l_send, l_recv,
                  far_send, far_recv, on_send, on_recv, own_sem):
    x, z, c, y = place()
    steps, mates = row_mates(x, z, c, y)
    mate = dict(zip(steps, mates))
    greet(mates)
    keep = [pltpu.make_async_copy(o_ref.at[x, c], o_all.at[x, c], own_sem.at[0]),
            pltpu.make_async_copy(lse_ref.at[x, c], lse_all.at[x, c], own_sem.at[1])]
    copies, far = [], []
    for side, dx in ((0, 1), (1, 3)):
        for dc in range(2):
            far.append(remote(o_ref.at[(x + 2) % ROW, (c + dc) % 2, side], relay.at[side, dc],
                              far_send.at[side, dc], far_recv.at[side, dc], mate[dx, 0]))
            far[-1].start()
    for n, (dx, dc) in enumerate(steps):
        to_x, to_c = (x + dx) % ROW, (c + dc) % 2
        copies.append(remote(lse_ref.at[to_x, to_c], lse_all.at[x, c], l_send.at[n], l_recv.at[n], mates[n]))
        copies[-1].start()
        if dx != 2:
            copies.append(remote(o_ref.at[to_x, to_c], o_all.at[x, c], o_send.at[n], o_recv.at[n], mates[n]))
            copies[-1].start()
    for copy in keep:
        copy.start()
    for k, (side, dx) in enumerate(((0, 1), (1, 3))):
        for dc in range(2):
            far[2 * k + dc].wait()
            copies.append(remote(relay.at[side, dc], o_all.at[(x + ROW - dx) % ROW, c, side],
                                 on_send.at[side, dc], on_recv.at[side, dc], mate[dx, dc]))
            copies[-1].start()
    for copy in [*keep, *copies]:
        copy.wait()


def send_back(o, lse):
    sem = pltpu.SemaphoreType.DMA
    vmem = pl.BlockSpec(memory_space=pltpu.VMEM)
    n = 2 * ROW - 1
    return pl.pallas_call(
        return_kernel,
        out_shape=(jax.ShapeDtypeStruct(o.shape, o.dtype), jax.ShapeDtypeStruct(lse.shape, lse.dtype)),
        in_specs=[vmem, vmem],
        out_specs=(vmem, vmem),
        scratch_shapes=[pltpu.VMEM((2, 2, *o.shape[-2:]), o.dtype),
                        sem((n,)), sem((n,)), sem((n,)), sem((n,)),
                        sem((2, 2)), sem((2, 2)), sem((2, 2)), sem((2, 2)), sem((2,))],
        compiler_params=pltpu.CompilerParams(
            collective_id=1, has_side_effects=True, vmem_limit_bytes=32 * 1024 * 1024),
        cost_estimate=pl.CostEstimate(flops=0, bytes_accessed=20_000_000, transcendentals=0),
    )(o, lse)


def body(stored_query_rows, stored_key_rows, stored_value_rows, span_order):
    rows, heads, width = stored_query_rows.shape
    span = rows // EACH
    q = stored_query_rows.reshape(EACH, span, 2, 2, 2, width).transpose(2, 3, 0, 4, 1, 5)
    q = q.reshape(2, 2, EACH, 2 * span, width)
    kv = jnp.stack([stored_key_rows, stored_value_rows])
    kv = kv.reshape(2, EACH, 2, span // 2, 2, width).transpose(4, 2, 0, 1, 3, 5)
    kv = kv.reshape(4, 2, EACH, span // 2, width)
    places = span_order.astype(jnp.float32).reshape(RING // 2, 2, ROW, 2, EACH).transpose(0, 3, 1, 2, 4)
    places = jnp.broadcast_to(places.reshape(RING, 2 * ROW * EACH, 1), (RING, 2 * ROW * EACH, 2 * span))
    o, lse = finish(places, span_order, *attend(places, q, kv))

    o, lse = send_back(o.reshape(ROW, 2, EACH, 2 * span, width), lse.reshape(ROW, 2, EACH, 1, 2 * span))
    o = o.reshape(2, 2, 2, EACH, 2, span, width)
    lse = lse.reshape(2, 2, 2, EACH, 2, span)
    top = jnp.max(lse, axis=0)
    weights = jnp.exp2(lse - top)
    share = weights / jnp.sum(weights, axis=0)
    result = jnp.sum(o.astype(jnp.float32) * share[..., None], axis=0).astype(jnp.bfloat16)
    return result.transpose(2, 4, 0, 1, 3, 5).reshape(rows, heads, width)


def solution(mesh):
    placed = (
        P(("outer", "inner"), "head", None),
        P(("outer", "inner"), "head", None),
        P(("outer", "inner"), "head", None),
        P(),
    )
    return jax.shard_map(
        body,
        mesh=mesh,
        in_specs=placed,
        out_specs=P(("outer", "inner"), "head", None),
        check_vma=False,
    )
```

```python
import math

import jax
import jax.numpy as jnp
from jax import lax
from jax.experimental import pallas as pl
from jax.experimental.pallas import tpu as pltpu
from jax.sharding import PartitionSpec as P

ROW = 4
RING = 8
EACH = 2
NEAR = 3
MESH = pl.DeviceIdType.MESH
NEVER = 2.0**20


def place():
    outer, inner = lax.axis_index("outer"), lax.axis_index("inner")
    return inner // 2, outer // 2 * 2 + inner % 2, outer % 2, lax.axis_index("head")


def device(x, z, c, y):
    return (z // 2 * 2 + c, x * 2 + z % 2, y)


def greet(peers):
    barrier = pltpu.get_barrier_semaphore()
    for peer in peers:
        pl.semaphore_signal(barrier, inc=1, device_id=peer, device_id_type=MESH)
    pl.semaphore_wait(barrier, len(peers))


def row_mates(x, z, c, y):
    steps = [(dx, dc) for dx in range(ROW) for dc in range(2) if (dx, dc) != (0, 0)]
    return steps, [device((x + dx) % ROW, z, (c + dc) % 2, y) for dx, dc in steps]


def remote(src, dst, send, recv, to):
    return pltpu.make_async_remote_copy(
        src_ref=src, dst_ref=dst, send_sem=send, recv_sem=recv, device_id=to, device_id_type=MESH)


def attend_kernel(place_ref, q_ref, kv_ref, q_all, kv_all, acc, total, top, q_turned, marks,
                  v_turned, p_bufs, relay,
                  q_send, q_recv, far_send, far_recv, on_send, on_recv, x_send, x_recv,
                  up_send, up_recv, down_send, down_recv, core_send, core_recv, own_sem):
    x, z, c, y = place()
    steps, mates = row_mates(x, z, c, y)
    mate = dict(zip(steps, mates))
    above, below = device(x, (z + 1) % RING, c, y), device(x, (z + RING - 1) % RING, c, y)
    partner = mate[0, 1]
    greet([*mates, above, below])
    piece, width = kv_ref.shape[-2:]
    block = 2 * piece
    lanes = q_ref.shape[-2]
    tiles = 2 * ROW * EACH
    window = 2 * ROW * EACH * piece
    rate = math.log2(math.e) / math.sqrt(width)
    half = x // 2
    role = x % 2 * 2 + x // 2
    mine = kv_ref.at[role]

    def slot_of(off, j):
        return kv_all.at[c, (z + off + RING) % RING, (x + j) % ROW]

    def pass_up(t, j, src):
        remote(src, slot_of(-t, j), up_send.at[t, j], up_recv.at[t, j], above).start()

    def pass_down(t, j, src):
        remote(src, slot_of(t, j), down_send.at[t, j], down_recv.at[t, j], below).start()

    def to_partner(off, j, src):
        r = (off + RING) % RING
        remote(src, slot_of(off, j), core_send.at[r, j], core_recv.at[r, j], partner).start()

    def arrived(dst, recv):
        remote(dst, dst, x_send.at[1], recv, partner).wait_recv()

    def gone(src, send):
        remote(src, src, send, x_recv.at[1], partner).wait_send()

    pass_up(0, 0, mine)
    pass_down(0, 0, mine)
    for d in (1, 3, 2):
        to = (x + d) % ROW
        remote(kv_ref.at[to % 2 * 2 + to // 2], kv_all.at[c, z, x], x_send.at[d], x_recv.at[d],
               device(to, z, c, y)).start()
    to_partner(0, 0, mine)
    keep_kv = pltpu.make_async_copy(mine, kv_all.at[c, z, x], own_sem.at[0])
    keep_q = pltpu.make_async_copy(q_ref.at[x % 2, c], q_all.at[x, c], own_sem.at[1])
    keep_kv.start()
    keep_q.start()
    for n, (dx, dc) in enumerate(steps):
        if dx != 2:
            remote(q_ref.at[(x + dx) % 2, (c + dc) % 2], q_all.at[x, c], q_send.at[n], q_recv.at[n],
                   mates[n]).start()
    for side, dx in ((0, 1), (1, 3)):
        for dc in range(2):
            remote(q_ref.at[x % 2, (c + dc) % 2, side], relay.at[side, dc], far_send.at[side, dc],
                   far_recv.at[side, dc], mate[dx, 0]).start()

    k_row = lax.broadcasted_iota(jnp.int32, (window, width), 0)
    column = lax.broadcasted_iota(jnp.int32, (window, width), 1)
    marks[...] = jnp.where((column == k_row // piece) | (column == tiles), 1.0, 0.0).astype(marks.dtype)
    q_turned[:, width + tiles:, :] = jnp.zeros((tiles, width - tiles, lanes), q_turned.dtype)

    for j in (1, 3, 2):
        slot = slot_of(0, j)
        arrived(slot, x_recv.at[ROW - j])
        pass_up(0, j, slot)
        pass_down(0, j, slot)
        to_partner(0, j, slot)
    keep_kv.wait()
    keep_q.wait()

    def forward():
        for side, dx in ((0, 1), (1, 3)):
            for dc in range(2):
                arrived(relay.at[side, dc], far_recv.at[side, dc])
                remote(relay.at[side, dc], q_all.at[(x + ROW - dx) % ROW, c, side], on_send.at[side, dc],
                       on_recv.at[side, dc], mate[dx, dc]).start()

    def ready(zc):
        r = (zc - z + RING) % RING
        for j in range(ROW):
            arrived(kv_all.at[1 - c, zc, (x + j) % ROW], core_recv.at[r, j])
        for core in range(2):
            for at in range(ROW):
                v = kv_all[core, zc, at, 1].reshape(EACH * piece, width)
                v_turned[(core * RING + zc) * ROW + at] = v.T

    ready(z)

    own_k = lax.broadcasted_iota(jnp.int32, (piece, lanes), 0) + half * piece
    own_allowed = own_k <= lax.broadcasted_iota(jnp.int32, (piece, lanes), 1) % block

    def take(at, core):
        for b in range(EACH):
            t = (at * 2 + core) * EACH + b
            q = q_all[at, core, b].T
            q_turned[t, :width, :] = q
            s = jnp.dot(kv_all[core, z, at, 0, b], q, preferred_element_type=jnp.float32)
            ref = jnp.max(s, axis=0, keepdims=True).astype(jnp.bfloat16).astype(jnp.float32)
            top[t] = ref
            first = lax.broadcasted_iota(jnp.int32, (tiles, lanes), 0) == 0
            q_turned[t, width + tiles:width + 2 * tiles, :] = jnp.where(first, -ref, 0.0).astype(q_turned.dtype)
            p = jnp.where(own_allowed, jnp.exp2((s - ref) * rate), 0.0)
            total[t] = jnp.sum(p.reshape(piece // 8, 8, lanes), axis=0)
            v = v_turned[(core * RING + z) * ROW + at]
            acc[t] = jnp.dot(v[:, b * piece:(b + 1) * piece], p.astype(jnp.bfloat16), preferred_element_type=jnp.float32)

    take(x, c)
    arrived(q_all.at[x, 1 - c], q_recv.at[steps.index((0, 1))])
    take(x, 1 - c)

    def await_queries(dx):
        for core in range(2):
            if dx == 2:
                for side in range(2):
                    dc = (core + c) % 2
                    arrived(q_all.at[(x + 2) % ROW, core, side], on_recv.at[side, dc])
            else:
                dc = (core + c) % 2
                arrived(q_all.at[(x + ROW - dx) % ROW, core], q_recv.at[steps.index((dx, 0)) + dc])

    def row_at(n):
        off = jnp.where(n % 2 == 1, -((n + 1) // 2), n // 2)
        return off, (z + off + RING) % RING

    def weigh(t, zc, buf):
        own = (t // EACH % 2 * ROW + t // (2 * EACH)) * EACH + t % EACH
        before = place_ref[zc] < place_ref[z, pl.ds(own, 1), :]
        q_turned[t, width:width + tiles, :] = jnp.where(before, 0.0, -NEVER).astype(q_turned.dtype)
        k = [kv_all[core, zc, at, 0].reshape(EACH * piece, width) for core in range(2) for at in range(ROW)]
        keys = jnp.concatenate([jnp.concatenate(k, axis=0), marks[...]], axis=1)
        s = jnp.dot(keys, q_turned[t], preferred_element_type=jnp.float32)
        p = jnp.exp2(s * rate)
        total[t] += jnp.sum(p.reshape(window // 8, 8, lanes), axis=0)
        p_bufs[buf][...] = p.astype(jnp.bfloat16)

    def absorb(t, zc, buf):
        v = [v_turned[(core * RING + zc) * ROW + at] for core in range(2) for at in range(ROW)]
        acc[t] += jnp.dot(jnp.concatenate(v, axis=1), p_bufs[buf][...], preferred_element_type=jnp.float32)

    def rise(t, j):
        slot = slot_of(-t, j)
        arrived(slot, up_recv.at[t - 1, j])

        @pl.when((t < 3) | ((t == 3) & (j < 2)))
        def _():
            pass_up(t, j, slot)

        to_partner(-t, j, slot)

    def fall(t, j):
        slot = slot_of(t, j)
        arrived(slot, down_recv.at[t - 1, j])

        @pl.when((t < 3) | ((t == 3) & (j >= 2)))
        def _():
            pass_down(t, j, slot)

        to_partner(t, j, slot)

    for j in (0, 1, 3, 2):
        rise(1, j)
        fall(1, j)

    per_turn = 2 * EACH
    turns = ROW * NEAR

    def plan(m):
        g = m // NEAR
        chip = (x + jnp.where(g == 1, 3, jnp.where(g == 2, 1, jnp.where(g == 3, 2, 0)))) % ROW
        return chip, chip * per_turn, row_at(m % NEAR)[1]

    def turn(m, carry):
        _, base, zc = plan(m)
        chip, next_base, next_zc = plan(m + 1)

        @pl.when(m < NEAR - 1)
        def _():
            ready(next_zc)

        @pl.when((m >= NEAR) & (m < NEAR + 2 * ROW))
        def _():
            event = m - NEAR
            t, j = event // ROW + 2, event % ROW
            j = jnp.where(j == 2, 3, jnp.where(j == 3, 2, j))
            rise(t, j)
            fall(t, j)

        for g, dx in ((1, 1), (2, 3), (3, 2)):
            @pl.when(m == NEAR * g - 1)
            def _(dx=dx):
                await_queries(dx)

        @pl.when(m == NEAR + 1)
        def _():
            forward()

        @pl.when((m == NEAR - 1) | (m == 2 * NEAR - 1) | (m == 3 * NEAR - 1))
        def _():
            take(chip, 0)
            take(chip, 1)

        for u in range(per_turn):
            done = u == per_turn - 1
            weigh(next_base if done else base + u + 1, next_zc if done else zc, 1 - u % 2)
            absorb(base + u, zc, u % 2)
        return carry

    weigh(x * per_turn, z, 0)
    lax.fori_loop(0, turns - 1, turn, 0)
    for up_j, down_j in ((0, 3), (1, 2)):
        rise(RING // 2, up_j)
        fall(RING // 2, down_j)
    _, last_base, last_zc = plan(turns - 1)
    for u in range(per_turn):
        if u < per_turn - 1:
            weigh(last_base + u + 1, last_zc, 1 - u % 2)
        absorb(last_base + u, last_zc, u % 2)
    for r in range(2, RING - 1):
        for j in range(ROW):
            arrived(kv_all.at[1 - c, (z + r) % RING, (x + j) % ROW], core_recv.at[r, j])

    for j in range(ROW):
        for t in range(RING // 2):
            if t < 3 or j < 2:
                gone(slot_of(0, j), up_send.at[t, j])
            if t < 3 or j >= 2:
                gone(slot_of(0, j), down_send.at[t, j])
        for r in range(RING):
            gone(slot_of(0, j), core_send.at[r, j])
        if j:
            gone(slot_of(0, j), x_send.at[j])
    for side in range(2):
        for dc in range(2):
            gone(relay.at[side, dc], far_send.at[side, dc])
            gone(relay.at[side, dc], on_send.at[side, dc])
    for n, (dx, dc) in enumerate(steps):
        if dx != 2:
            gone(q_all.at[x, c], q_send.at[n])


def attend(places, q, kv):
    sem = pltpu.SemaphoreType.DMA
    half_ring = RING // 2
    vmem = pl.BlockSpec(memory_space=pltpu.VMEM)
    lanes, width = q.shape[-2:]
    piece = kv.shape[-2]
    tiles = 2 * ROW * EACH
    window = tiles * piece
    return pl.pallas_call(
        attend_kernel,
        out_shape=(jax.ShapeDtypeStruct((ROW, 2, *q.shape[2:]), q.dtype),
                   jax.ShapeDtypeStruct((2, RING, ROW, *kv.shape[1:]), kv.dtype),
                   jax.ShapeDtypeStruct((tiles, width, lanes), jnp.float32),
                   jax.ShapeDtypeStruct((tiles, 8, lanes), jnp.float32),
                   jax.ShapeDtypeStruct((tiles, 1, lanes), jnp.float32),
                   jax.ShapeDtypeStruct((tiles, 2 * width, lanes), jnp.bfloat16),
                   jax.ShapeDtypeStruct((window, width), jnp.bfloat16)),
        in_specs=[vmem] * 3,
        out_specs=(vmem,) * 7,
        scratch_shapes=[
            pltpu.VMEM((2 * RING * ROW, width, width), jnp.bfloat16),
            [pltpu.VMEM((window, lanes), jnp.bfloat16)] * 2,
            pltpu.VMEM((2, 2, lanes, width), jnp.bfloat16),
            sem((2 * ROW - 1,)), sem((2 * ROW - 1,)), sem((2, 2)), sem((2, 2)), sem((2, 2)), sem((2, 2)),
            sem((ROW,)), sem((ROW,)),
            sem((half_ring, ROW)), sem((half_ring, ROW)), sem((half_ring, ROW)), sem((half_ring, ROW)),
            sem((RING, ROW)), sem((RING, ROW)), sem((2,)),
        ],
        compiler_params=pltpu.CompilerParams(
            collective_id=0, has_side_effects=True, vmem_limit_bytes=32 * 1024 * 1024),
        cost_estimate=pl.CostEstimate(flops=10**10, bytes_accessed=20_000_000, transcendentals=0),
    )(places, q, kv)


def finish_kernel(place_ref, order, rank, q_all, kv_all, acc, total, top, q_turned, marks, o_ref, lse_ref,
                  k_sorted, v_sorted, v_turned, p_bufs, far_acc, far_total, again_acc, again_top):
    x, z, _, _ = place()
    half = x // 2
    tiles, _, lanes = acc.shape
    piece, width = kv_all.shape[-2:]
    block = 2 * piece
    rate = math.log2(math.e) / math.sqrt(width)
    q_row = lax.broadcasted_iota(jnp.int32, (1, lanes), 1) % block

    def stored(zc, core, at, b):
        return order[((zc // 2 * 2 + core) * RING + at * 2 + zc % 2) * EACH + b]

    def put(t, weight, sums, reference):
        some = weight > 0
        weight = jnp.where(some, weight, 1.0)
        o_ref[t] = (sums * (1.0 / weight)).T.astype(jnp.bfloat16)
        lse_ref[t] = jnp.where(some, reference + jnp.log2(weight), -1e30)

    window = marks.shape[0]
    per_window = window // piece

    def sort(i, carry):
        n, g = i // (2 * ROW), i % (2 * ROW)
        off = jnp.where(n % 2 == 1, (n + 3) // 2, -((n + 4) // 2))
        zc = (z + off + RING) % RING
        core, at_x = g // ROW, g % ROW
        for b in range(EACH):
            at = pl.multiple_of(rank[((zc * 2 + core) * ROW + at_x) * EACH + b] * piece, piece)
            k_sorted[pl.ds(at, piece), :] = kv_all[core, zc, at_x, 0, b]
            v_sorted[pl.ds(at, piece), :] = kv_all[core, zc, at_x, 1, b]
        return carry

    lax.fori_loop(0, (RING - NEAR) * 2 * ROW, sort, 0, unroll=4)

    def turn(g, carry):
        at = pl.multiple_of(g * width, width)
        v_turned[g] = v_sorted[pl.ds(at, width), :].T
        return carry

    lax.fori_loop(0, v_turned.shape[0], turn, 0, unroll=8)

    def own_row(t):
        return (t // EACH % 2 * ROW + t // (2 * EACH)) * EACH + t % EACH

    def count_of(t):
        held = rank[z * tiles + own_row(jnp.minimum(t, tiles - 1))]
        return jnp.where(t < tiles, held, 0)

    def clear(t, items):
        far_acc[t] = jnp.zeros(far_acc.shape[1:], jnp.float32)
        far_total[t] = jnp.zeros(far_total.shape[1:], jnp.float32)
        return items + jnp.maximum((count_of(t) + per_window - 1) // per_window, 1)

    items = lax.fori_loop(0, tiles, clear, 0)
    block_row = lax.broadcasted_iota(jnp.int32, (tiles, lanes), 0)

    def weigh(t, w, buf):
        count, t = count_of(t), jnp.minimum(t, tiles - 1)
        at = pl.multiple_of(w * window, window)
        mask = jnp.where(block_row < count - w * per_window, 0.0, -NEVER).astype(q_turned.dtype)
        right = jnp.concatenate([q_turned[t, :width, :], mask, q_turned[t, width + tiles:, :]], axis=0)
        keys = jnp.concatenate([k_sorted[pl.ds(at, window), :], marks[...]], axis=1)
        p = jnp.exp2(jnp.dot(keys, right, preferred_element_type=jnp.float32) * rate)
        far_total[t] += jnp.sum(p.reshape(window // 8, 8, lanes), axis=0)
        p_bufs[buf][...] = p.astype(jnp.bfloat16)

    def absorb(t, w, buf):
        t = jnp.minimum(t, tiles - 1)
        v = [v_turned[w * (window // width) + i] for i in range(window // width)]
        far_acc[t] += jnp.dot(jnp.concatenate(v, axis=1), p_bufs[buf][...], preferred_element_type=jnp.float32)

    unroll = 4

    def step(i, at):
        t, w = at
        for u in range(unroll):
            last = (w + 1) * per_window >= count_of(t)
            next_t, next_w = jnp.where(last, t + 1, t), jnp.where(last, 0, w + 1)
            weigh(next_t, next_w, 1 - u % 2)
            absorb(t, w, u % 2)
            t, w = next_t, next_w
        return t, w

    weigh(jnp.int32(0), jnp.int32(0), 0)
    lax.fori_loop(0, (items + unroll - 1) // unroll, step, (jnp.int32(0), jnp.int32(0)))

    worst = jnp.zeros((1, lanes), jnp.float32)
    for t in range(tiles):
        weight = jnp.sum(total[t] + far_total[t], axis=0, keepdims=True)
        own = own_row(t)
        no_key = (place_ref[z, own:own + 1, :] == 0) & (q_row < half * piece)
        fits = ((weight > 2.0**-60) & (weight < 2.0**80)) | no_key
        worst = jnp.maximum(worst, jnp.where(fits, 0.0, 1.0))
        put(t, weight, acc[t] + far_acc[t], top[t] * rate)

    def redo(t, carry):
        at_q, core_q, b_q = t // (2 * EACH), t // EACH % 2, t % EACH
        pos = stored(z, core_q, at_q, b_q)
        q = q_all[at_q, core_q, b_q].T
        again_acc[...] = jnp.zeros_like(again_acc)
        again_top[0:1, :] = jnp.full((1, lanes), -1e30, jnp.float32)
        again_top[1:2, :] = jnp.zeros((1, lanes), jnp.float32)

        def one(g, carry):
            core, zc, at = g // (RING * ROW), g // ROW % RING, g % ROW
            for b in range(EACH):
                kp = stored(zc, core, at, b)
                k_at = lax.broadcasted_iota(jnp.int32, (piece, lanes), 0) + half * piece + kp * block
                s = jnp.dot(kv_all[core, zc, at, 0, b], q, preferred_element_type=jnp.float32) * rate
                s = jnp.where(k_at <= pos * block + q_row, s, -2e30)
                old = again_top[0:1, :]
                new = jnp.maximum(old, jnp.max(s, axis=0, keepdims=True))
                p = jnp.exp2(s - new)
                fade = jnp.exp2(old - new)
                again_top[0:1, :] = new
                again_top[1:2, :] = again_top[1:2, :] * fade + jnp.sum(p, axis=0, keepdims=True)
                v = kv_all[core, zc, at, 1, b].T
                again_acc[...] = again_acc[...] * fade + jnp.dot(
                    v, p.astype(jnp.bfloat16), preferred_element_type=jnp.float32)
            return carry

        lax.fori_loop(0, 2 * RING * ROW, one, 0)
        put(t, again_top[1:2, :], again_acc[...], again_top[0:1, :])
        return carry

    @pl.when(jnp.max(worst) > 0)
    def _():
        lax.fori_loop(0, tiles, redo, 0)


def finish(places, order, rank, q_all, kv_all, acc, total, top, q_turned, marks):
    smem = pl.BlockSpec(memory_space=pltpu.SMEM)
    vmem = pl.BlockSpec(memory_space=pltpu.VMEM)
    tiles, width, lanes = acc.shape
    far = (RING - NEAR) * 2 * ROW * EACH * kv_all.shape[-2]
    return pl.pallas_call(
        finish_kernel,
        out_shape=(jax.ShapeDtypeStruct((tiles, lanes, width), jnp.bfloat16),
                   jax.ShapeDtypeStruct((tiles, 1, lanes), jnp.float32)),
        in_specs=[vmem, smem, smem, *[vmem] * 7],
        out_specs=(vmem, vmem),
        scratch_shapes=[
            pltpu.VMEM((far, width), jnp.bfloat16),
            pltpu.VMEM((far, width), jnp.bfloat16),
            pltpu.VMEM((far // width, width, width), jnp.bfloat16),
            [pltpu.VMEM((marks.shape[0], lanes), jnp.bfloat16)] * 2,
            pltpu.VMEM(acc.shape, jnp.float32),
            pltpu.VMEM(total.shape, jnp.float32),
            pltpu.VMEM((width, lanes), jnp.float32),
            pltpu.VMEM((8, lanes), jnp.float32),
        ],
        compiler_params=pltpu.CompilerParams(vmem_limit_bytes=28 * 1024 * 1024),
    )(places, order, rank, q_all, kv_all, acc, total, top, q_turned, marks)


def return_kernel(o_ref, lse_ref, o_all, lse_all, relay, o_send, o_recv, l_send, l_recv,
                  far_send, far_recv, on_send, on_recv, own_sem):
    x, z, c, y = place()
    steps, mates = row_mates(x, z, c, y)
    mate = dict(zip(steps, mates))
    greet(mates)
    keep = [pltpu.make_async_copy(o_ref.at[x, c], o_all.at[x, c], own_sem.at[0]),
            pltpu.make_async_copy(lse_ref.at[x, c], lse_all.at[x, c], own_sem.at[1])]
    copies, far = [], []
    for side, dx in ((0, 1), (1, 3)):
        for dc in range(2):
            far.append(remote(o_ref.at[(x + 2) % ROW, (c + dc) % 2, side], relay.at[side, dc],
                              far_send.at[side, dc], far_recv.at[side, dc], mate[dx, 0]))
            far[-1].start()
    for n, (dx, dc) in enumerate(steps):
        to_x, to_c = (x + dx) % ROW, (c + dc) % 2
        copies.append(remote(lse_ref.at[to_x, to_c], lse_all.at[x, c], l_send.at[n], l_recv.at[n], mates[n]))
        copies[-1].start()
        if dx != 2:
            copies.append(remote(o_ref.at[to_x, to_c], o_all.at[x, c], o_send.at[n], o_recv.at[n], mates[n]))
            copies[-1].start()
    for copy in keep:
        copy.start()
    for k, (side, dx) in enumerate(((0, 1), (1, 3))):
        for dc in range(2):
            far[2 * k + dc].wait()
            copies.append(remote(relay.at[side, dc], o_all.at[(x + ROW - dx) % ROW, c, side],
                                 on_send.at[side, dc], on_recv.at[side, dc], mate[dx, dc]))
            copies[-1].start()
    for copy in [*keep, *copies]:
        copy.wait()


def send_back(o, lse):
    sem = pltpu.SemaphoreType.DMA
    vmem = pl.BlockSpec(memory_space=pltpu.VMEM)
    n = 2 * ROW - 1
    return pl.pallas_call(
        return_kernel,
        out_shape=(jax.ShapeDtypeStruct(o.shape, o.dtype), jax.ShapeDtypeStruct(lse.shape, lse.dtype)),
        in_specs=[vmem, vmem],
        out_specs=(vmem, vmem),
        scratch_shapes=[pltpu.VMEM((2, 2, *o.shape[-2:]), o.dtype),
                        sem((n,)), sem((n,)), sem((n,)), sem((n,)),
                        sem((2, 2)), sem((2, 2)), sem((2, 2)), sem((2, 2)), sem((2,))],
        compiler_params=pltpu.CompilerParams(
            collective_id=1, has_side_effects=True, vmem_limit_bytes=32 * 1024 * 1024),
        cost_estimate=pl.CostEstimate(flops=0, bytes_accessed=20_000_000, transcendentals=0),
    )(o, lse)


def body(stored_query_rows, stored_key_rows, stored_value_rows, span_order):
    rows, heads, width = stored_query_rows.shape
    span = rows // EACH
    q = stored_query_rows.reshape(EACH, span, 2, 2, 2, width).transpose(2, 3, 0, 4, 1, 5)
    q = q.reshape(2, 2, EACH, 2 * span, width)
    kv = jnp.stack([stored_key_rows, stored_value_rows])
    kv = kv.reshape(2, EACH, 2, span // 2, 2, width).transpose(4, 2, 0, 1, 3, 5)
    kv = kv.reshape(4, 2, EACH, span // 2, width)
    places = span_order.astype(jnp.float32).reshape(RING // 2, 2, ROW, 2, EACH).transpose(0, 3, 1, 2, 4)
    flat = places.reshape(-1)
    places = jnp.broadcast_to(places.reshape(RING, 2 * ROW * EACH, 1), (RING, 2 * ROW * EACH, 2 * span))
    away = (jnp.arange(flat.shape[0]) // (2 * ROW * EACH) - place()[1] + RING + NEAR // 2) % RING >= NEAR
    rank = jnp.sum((away[None, :] & (flat[None, :] < flat[:, None])).astype(jnp.int32), axis=1)
    o, lse = finish(places, span_order, rank, *attend(places, q, kv))

    o, lse = send_back(o.reshape(ROW, 2, EACH, 2 * span, width), lse.reshape(ROW, 2, EACH, 1, 2 * span))
    o = o.reshape(2, 2, 2, EACH, 2, span, width)
    lse = lse.reshape(2, 2, 2, EACH, 2, span)
    top = jnp.max(lse, axis=0)
    weights = jnp.exp2(lse - top)
    share = weights / jnp.sum(weights, axis=0)
    result = jnp.sum(o.astype(jnp.float32) * share[..., None], axis=0).astype(jnp.bfloat16)
    return result.transpose(2, 4, 0, 1, 3, 5).reshape(rows, heads, width)


def solution(mesh):
    placed = (
        P(("outer", "inner"), "head", None),
        P(("outer", "inner"), "head", None),
        P(("outer", "inner"), "head", None),
        P(),
    )
    return jax.shard_map(
        body,
        mesh=mesh,
        in_specs=placed,
        out_specs=P(("outer", "inner"), "head", None),
        check_vma=False,
    )
```

```python
import math

import jax
import jax.numpy as jnp
from jax import lax
from jax.experimental import pallas as pl
from jax.experimental.pallas import tpu as pltpu
from jax.sharding import PartitionSpec as P

ROW = 4
RING = 8
EACH = 2
NEAR = 2
MESH = pl.DeviceIdType.MESH
NEVER = 2.0**20


def place():
    outer, inner = lax.axis_index("outer"), lax.axis_index("inner")
    return inner // 2, outer // 2 * 2 + inner % 2, outer % 2, lax.axis_index("head")


def device(x, z, c, y):
    return (z // 2 * 2 + c, x * 2 + z % 2, y)


def row_at(z, n):
    return (z + jnp.where(n % 2 == 1, -((n + 1) // 2), n // 2) + RING) % RING


def greet(peers):
    barrier = pltpu.get_barrier_semaphore()
    for peer in peers:
        pl.semaphore_signal(barrier, inc=1, device_id=peer, device_id_type=MESH)
    pl.semaphore_wait(barrier, len(peers))


def row_mates(x, z, c, y):
    steps = [(dx, dc) for dx in range(ROW) for dc in range(2) if (dx, dc) != (0, 0)]
    return steps, [device((x + dx) % ROW, z, (c + dc) % 2, y) for dx, dc in steps]


def remote(src, dst, send, recv, to):
    return pltpu.make_async_remote_copy(
        src_ref=src, dst_ref=dst, send_sem=send, recv_sem=recv, device_id=to, device_id_type=MESH)


def attend_kernel(place_ref, q_ref, kv_ref, q_all, kv_all, acc, total, top, q_turned, marks,
                  v_turned, p_bufs, relay,
                  q_send, q_recv, far_send, far_recv, on_send, on_recv, x_send, x_recv,
                  up_send, up_recv, down_send, down_recv, core_send, core_recv, own_sem):
    x, z, c, y = place()
    steps, mates = row_mates(x, z, c, y)
    mate = dict(zip(steps, mates))
    above, below = device(x, (z + 1) % RING, c, y), device(x, (z + RING - 1) % RING, c, y)
    partner = mate[0, 1]
    greet([*mates, above, below])
    piece, width = kv_ref.shape[-2:]
    block = 2 * piece
    lanes = q_ref.shape[-2]
    tiles = 2 * ROW * EACH
    window = 2 * ROW * EACH * piece
    rate = math.log2(math.e) / math.sqrt(width)
    half = x // 2
    role = x % 2 * 2 + x // 2
    mine = kv_ref.at[role]

    def slot_of(off, j):
        return kv_all.at[c, (z + off + RING) % RING, (x + j) % ROW]

    def pass_up(t, j, src):
        remote(src, slot_of(-t, j), up_send.at[t, j], up_recv.at[t, j], above).start()

    def pass_down(t, j, src):
        remote(src, slot_of(t, j), down_send.at[t, j], down_recv.at[t, j], below).start()

    def to_partner(off, j, src):
        r = (off + RING) % RING
        remote(src, slot_of(off, j), core_send.at[r, j], core_recv.at[r, j], partner).start()

    def arrived(dst, recv):
        remote(dst, dst, x_send.at[1], recv, partner).wait_recv()

    def gone(src, send):
        remote(src, src, send, x_recv.at[1], partner).wait_send()

    pass_up(0, 0, mine)
    pass_down(0, 0, mine)
    for d in (1, 3, 2):
        to = (x + d) % ROW
        remote(kv_ref.at[to % 2 * 2 + to // 2], kv_all.at[c, z, x], x_send.at[d], x_recv.at[d],
               device(to, z, c, y)).start()
    to_partner(0, 0, mine)
    keep_kv = pltpu.make_async_copy(mine, kv_all.at[c, z, x], own_sem.at[0])
    keep_q = pltpu.make_async_copy(q_ref.at[x % 2, c], q_all.at[x, c], own_sem.at[1])
    keep_kv.start()
    keep_q.start()
    for n, (dx, dc) in enumerate(steps):
        if dx != 2:
            remote(q_ref.at[(x + dx) % 2, (c + dc) % 2], q_all.at[x, c], q_send.at[n], q_recv.at[n],
                   mates[n]).start()
    for side, dx in ((0, 1), (1, 3)):
        for dc in range(2):
            remote(q_ref.at[x % 2, (c + dc) % 2, side], relay.at[side, dc], far_send.at[side, dc],
                   far_recv.at[side, dc], mate[dx, 0]).start()

    k_row = lax.broadcasted_iota(jnp.int32, (window, width), 0)
    column = lax.broadcasted_iota(jnp.int32, (window, width), 1)
    marks[...] = jnp.where((column == k_row // piece) | (column == tiles), 1.0, 0.0).astype(marks.dtype)
    q_turned[:, width + tiles:, :] = jnp.zeros((tiles, width - tiles, lanes), q_turned.dtype)

    for j in (1, 3, 2):
        slot = slot_of(0, j)
        arrived(slot, x_recv.at[ROW - j])
        pass_up(0, j, slot)
        pass_down(0, j, slot)
        to_partner(0, j, slot)
    keep_kv.wait()
    keep_q.wait()

    def forward():
        for side, dx in ((0, 1), (1, 3)):
            for dc in range(2):
                arrived(relay.at[side, dc], far_recv.at[side, dc])
                remote(relay.at[side, dc], q_all.at[(x + ROW - dx) % ROW, c, side], on_send.at[side, dc],
                       on_recv.at[side, dc], mate[dx, dc]).start()

    def ready(zc):
        r = (zc - z + RING) % RING
        for j in range(ROW):
            arrived(kv_all.at[1 - c, zc, (x + j) % ROW], core_recv.at[r, j])
        for core in range(2):
            for at in range(ROW):
                v = kv_all[core, zc, at, 1].reshape(EACH * piece, width)
                v_turned[(core * RING + zc) * ROW + at] = v.T

    ready(z)

    own_k = lax.broadcasted_iota(jnp.int32, (piece, lanes), 0) + half * piece
    own_allowed = own_k <= lax.broadcasted_iota(jnp.int32, (piece, lanes), 1) % block

    def take(at, core):
        for b in range(EACH):
            t = (at * 2 + core) * EACH + b
            q = q_all[at, core, b].T
            q_turned[t, :width, :] = q
            s = jnp.dot(kv_all[core, z, at, 0, b], q, preferred_element_type=jnp.float32)
            ref = jnp.max(s, axis=0, keepdims=True).astype(jnp.bfloat16).astype(jnp.float32)
            top[t] = ref
            first = lax.broadcasted_iota(jnp.int32, (tiles, lanes), 0) == 0
            q_turned[t, width + tiles:width + 2 * tiles, :] = jnp.where(first, -ref, 0.0).astype(q_turned.dtype)
            p = jnp.where(own_allowed, jnp.exp2((s - ref) * rate), 0.0)
            total[t] = jnp.sum(p.reshape(piece // 8, 8, lanes), axis=0)
            v = v_turned[(core * RING + z) * ROW + at]
            acc[t] = jnp.dot(v[:, b * piece:(b + 1) * piece], p.astype(jnp.bfloat16), preferred_element_type=jnp.float32)

    take(x, c)
    arrived(q_all.at[x, 1 - c], q_recv.at[steps.index((0, 1))])
    take(x, 1 - c)

    def await_queries(dx):
        for core in range(2):
            if dx == 2:
                for side in range(2):
                    dc = (core + c) % 2
                    arrived(q_all.at[(x + 2) % ROW, core, side], on_recv.at[side, dc])
            else:
                dc = (core + c) % 2
                arrived(q_all.at[(x + ROW - dx) % ROW, core], q_recv.at[steps.index((dx, 0)) + dc])

    def weigh(t, zc, buf):
        own = (t // EACH % 2 * ROW + t // (2 * EACH)) * EACH + t % EACH
        before = place_ref[zc] < place_ref[z, pl.ds(own, 1), :]
        q_turned[t, width:width + tiles, :] = jnp.where(before, 0.0, -NEVER).astype(q_turned.dtype)
        k = [kv_all[core, zc, at, 0].reshape(EACH * piece, width) for core in range(2) for at in range(ROW)]
        keys = jnp.concatenate([jnp.concatenate(k, axis=0), marks[...]], axis=1)
        s = jnp.dot(keys, q_turned[t], preferred_element_type=jnp.float32)
        p = jnp.exp2(s * rate)
        total[t] += jnp.sum(p.reshape(window // 8, 8, lanes), axis=0)
        p_bufs[buf][...] = p.astype(jnp.bfloat16)

    def absorb(t, zc, buf):
        v = [v_turned[(core * RING + zc) * ROW + at] for core in range(2) for at in range(ROW)]
        acc[t] += jnp.dot(jnp.concatenate(v, axis=1), p_bufs[buf][...], preferred_element_type=jnp.float32)

    def rise(t, j):
        slot = slot_of(-t, j)
        arrived(slot, up_recv.at[t - 1, j])

        @pl.when((t < 3) | ((t == 3) & (j < 2)))
        def _():
            pass_up(t, j, slot)

        to_partner(-t, j, slot)

    def fall(t, j):
        slot = slot_of(t, j)
        arrived(slot, down_recv.at[t - 1, j])

        @pl.when((t < 3) | ((t == 3) & (j >= 2)))
        def _():
            pass_down(t, j, slot)

        to_partner(t, j, slot)

    for j in (0, 1, 3, 2):
        rise(1, j)
        fall(1, j)

    per_turn = 2 * EACH
    turns = ROW * NEAR
    within = min(turns - 1 - NEAR, 2 * ROW)

    def plan(m):
        g = m // NEAR
        chip = (x + jnp.where(g == 1, 3, jnp.where(g == 2, 1, jnp.where(g == 3, 2, 0)))) % ROW
        return chip, chip * per_turn, row_at(z, m % NEAR)

    def turn(m, carry):
        _, base, zc = plan(m)
        chip, next_base, next_zc = plan(m + 1)

        @pl.when(m < NEAR - 1)
        def _():
            ready(next_zc)

        @pl.when((m >= NEAR) & (m < NEAR + within))
        def _():
            event = m - NEAR
            t, j = event // ROW + 2, event % ROW
            j = jnp.where(j == 2, 3, jnp.where(j == 3, 2, j))
            rise(t, j)
            fall(t, j)

        for g, dx in ((1, 1), (2, 3), (3, 2)):
            @pl.when(m == NEAR * g - 1)
            def _(dx=dx):
                await_queries(dx)

        @pl.when(m == NEAR + 1)
        def _():
            forward()

        @pl.when((m == NEAR - 1) | (m == 2 * NEAR - 1) | (m == 3 * NEAR - 1))
        def _():
            take(chip, 0)
            take(chip, 1)

        for u in range(per_turn):
            done = u == per_turn - 1
            weigh(next_base if done else base + u + 1, next_zc if done else zc, 1 - u % 2)
            absorb(base + u, zc, u % 2)
        return carry

    weigh(x * per_turn, z, 0)
    lax.fori_loop(0, turns - 1, turn, 0)
    _, last_base, last_zc = plan(turns - 1)
    for u in range(per_turn):
        if u < per_turn - 1:
            weigh(last_base + u + 1, last_zc, 1 - u % 2)
        absorb(last_base + u, last_zc, u % 2)
    for event in range(within, 2 * ROW):
        for hop in (rise, fall):
            hop(event // ROW + 2, (0, 1, 3, 2)[event % ROW])
    for up_j, down_j in ((0, 3), (1, 2)):
        rise(RING // 2, up_j)
        fall(RING // 2, down_j)
    near = [(RING - (n + 1) // 2 if n % 2 else n // 2) % RING for n in range(NEAR)]
    for r in range(RING):
        if r not in near:
            for j in range(ROW):
                arrived(kv_all.at[1 - c, (z + r) % RING, (x + j) % ROW], core_recv.at[r, j])

    for j in range(ROW):
        for t in range(RING // 2):
            if t < 3 or j < 2:
                gone(slot_of(0, j), up_send.at[t, j])
            if t < 3 or j >= 2:
                gone(slot_of(0, j), down_send.at[t, j])
        for r in range(RING):
            gone(slot_of(0, j), core_send.at[r, j])
        if j:
            gone(slot_of(0, j), x_send.at[j])
    for side in range(2):
        for dc in range(2):
            gone(relay.at[side, dc], far_send.at[side, dc])
            gone(relay.at[side, dc], on_send.at[side, dc])
    for n, (dx, dc) in enumerate(steps):
        if dx != 2:
            gone(q_all.at[x, c], q_send.at[n])


def attend(places, q, kv):
    sem = pltpu.SemaphoreType.DMA
    half_ring = RING // 2
    vmem = pl.BlockSpec(memory_space=pltpu.VMEM)
    lanes, width = q.shape[-2:]
    piece = kv.shape[-2]
    tiles = 2 * ROW * EACH
    window = tiles * piece
    return pl.pallas_call(
        attend_kernel,
        out_shape=(jax.ShapeDtypeStruct((ROW, 2, *q.shape[2:]), q.dtype),
                   jax.ShapeDtypeStruct((2, RING, ROW, *kv.shape[1:]), kv.dtype),
                   jax.ShapeDtypeStruct((tiles, width, lanes), jnp.float32),
                   jax.ShapeDtypeStruct((tiles, 8, lanes), jnp.float32),
                   jax.ShapeDtypeStruct((tiles, 1, lanes), jnp.float32),
                   jax.ShapeDtypeStruct((tiles, 2 * width, lanes), jnp.bfloat16),
                   jax.ShapeDtypeStruct((window, width), jnp.bfloat16)),
        in_specs=[vmem] * 3,
        out_specs=(vmem,) * 7,
        scratch_shapes=[
            pltpu.VMEM((2 * RING * ROW, width, width), jnp.bfloat16),
            [pltpu.VMEM((window, lanes), jnp.bfloat16)] * 2,
            pltpu.VMEM((2, 2, lanes, width), jnp.bfloat16),
            sem((2 * ROW - 1,)), sem((2 * ROW - 1,)), sem((2, 2)), sem((2, 2)), sem((2, 2)), sem((2, 2)),
            sem((ROW,)), sem((ROW,)),
            sem((half_ring, ROW)), sem((half_ring, ROW)), sem((half_ring, ROW)), sem((half_ring, ROW)),
            sem((RING, ROW)), sem((RING, ROW)), sem((2,)),
        ],
        compiler_params=pltpu.CompilerParams(
            collective_id=0, has_side_effects=True, vmem_limit_bytes=32 * 1024 * 1024),
        cost_estimate=pl.CostEstimate(flops=10**10, bytes_accessed=20_000_000, transcendentals=0),
    )(places, q, kv)


def finish_kernel(place_ref, order, rank, q_all, kv_all, acc, total, top, q_turned, marks, o_ref, lse_ref,
                  k_sorted, v_sorted, v_turned, p_bufs, far_acc, far_total, again_acc, again_top):
    x, z, _, _ = place()
    half = x // 2
    tiles, _, lanes = acc.shape
    piece, width = kv_all.shape[-2:]
    block = 2 * piece
    rate = math.log2(math.e) / math.sqrt(width)
    q_row = lax.broadcasted_iota(jnp.int32, (1, lanes), 1) % block

    def stored(zc, core, at, b):
        return order[((zc // 2 * 2 + core) * RING + at * 2 + zc % 2) * EACH + b]

    def put(t, weight, sums, reference):
        some = weight > 0
        weight = jnp.where(some, weight, 1.0)
        o_ref[t] = (sums * (1.0 / weight)).T.astype(jnp.bfloat16)
        lse_ref[t] = jnp.where(some, reference + jnp.log2(weight), -1e30)

    window = marks.shape[0]
    per_window = window // piece

    def sort(i, carry):
        n, g = i // (2 * ROW), i % (2 * ROW)
        zc = row_at(z, n + NEAR)
        core, at_x = g // ROW, g % ROW
        for b in range(EACH):
            at = pl.multiple_of(rank[((zc * 2 + core) * ROW + at_x) * EACH + b] * piece, piece)
            k_sorted[pl.ds(at, piece), :] = kv_all[core, zc, at_x, 0, b]
            v_sorted[pl.ds(at, piece), :] = kv_all[core, zc, at_x, 1, b]
        return carry

    lax.fori_loop(0, (RING - NEAR) * 2 * ROW, sort, 0, unroll=4)

    def turn(g, carry):
        at = pl.multiple_of(g * width, width)
        v_turned[g] = v_sorted[pl.ds(at, width), :].T
        return carry

    lax.fori_loop(0, v_turned.shape[0], turn, 0, unroll=8)

    def own_row(t):
        return (t // EACH % 2 * ROW + t // (2 * EACH)) * EACH + t % EACH

    def count_of(t):
        held = rank[z * tiles + own_row(jnp.minimum(t, tiles - 1))]
        return jnp.where(t < tiles, held, 0)

    def clear(t, items):
        far_acc[t] = jnp.zeros(far_acc.shape[1:], jnp.float32)
        far_total[t] = jnp.zeros(far_total.shape[1:], jnp.float32)
        return items + jnp.maximum((count_of(t) + per_window - 1) // per_window, 1)

    items = lax.fori_loop(0, tiles, clear, 0)
    block_row = lax.broadcasted_iota(jnp.int32, (tiles, lanes), 0)

    def weigh(t, w, buf):
        count, t = count_of(t), jnp.minimum(t, tiles - 1)
        at = pl.multiple_of(w * window, window)
        mask = jnp.where(block_row < count - w * per_window, 0.0, -NEVER).astype(q_turned.dtype)
        right = jnp.concatenate([q_turned[t, :width, :], mask, q_turned[t, width + tiles:, :]], axis=0)
        keys = jnp.concatenate([k_sorted[pl.ds(at, window), :], marks[...]], axis=1)
        p = jnp.exp2(jnp.dot(keys, right, preferred_element_type=jnp.float32) * rate)
        far_total[t] += jnp.sum(p.reshape(window // 8, 8, lanes), axis=0)
        p_bufs[buf][...] = p.astype(jnp.bfloat16)

    def absorb(t, w, buf):
        t = jnp.minimum(t, tiles - 1)
        v = [v_turned[w * (window // width) + i] for i in range(window // width)]
        far_acc[t] += jnp.dot(jnp.concatenate(v, axis=1), p_bufs[buf][...], preferred_element_type=jnp.float32)

    unroll = 4

    def step(i, at):
        t, w = at
        for u in range(unroll):
            last = (w + 1) * per_window >= count_of(t)
            next_t, next_w = jnp.where(last, t + 1, t), jnp.where(last, 0, w + 1)
            weigh(next_t, next_w, 1 - u % 2)
            absorb(t, w, u % 2)
            t, w = next_t, next_w
        return t, w

    weigh(jnp.int32(0), jnp.int32(0), 0)
    lax.fori_loop(0, (items + unroll - 1) // unroll, step, (jnp.int32(0), jnp.int32(0)))

    worst = jnp.zeros((1, lanes), jnp.float32)
    for t in range(tiles):
        weight = jnp.sum(total[t] + far_total[t], axis=0, keepdims=True)
        own = own_row(t)
        no_key = (place_ref[z, own:own + 1, :] == 0) & (q_row < half * piece)
        fits = ((weight > 2.0**-60) & (weight < 2.0**80)) | no_key
        worst = jnp.maximum(worst, jnp.where(fits, 0.0, 1.0))
        put(t, weight, acc[t] + far_acc[t], top[t] * rate)

    def redo(t, carry):
        at_q, core_q, b_q = t // (2 * EACH), t // EACH % 2, t % EACH
        pos = stored(z, core_q, at_q, b_q)
        q = q_all[at_q, core_q, b_q].T
        again_acc[...] = jnp.zeros_like(again_acc)
        again_top[0:1, :] = jnp.full((1, lanes), -1e30, jnp.float32)
        again_top[1:2, :] = jnp.zeros((1, lanes), jnp.float32)

        def one(g, carry):
            core, zc, at = g // (RING * ROW), g // ROW % RING, g % ROW
            for b in range(EACH):
                kp = stored(zc, core, at, b)
                k_at = lax.broadcasted_iota(jnp.int32, (piece, lanes), 0) + half * piece + kp * block
                s = jnp.dot(kv_all[core, zc, at, 0, b], q, preferred_element_type=jnp.float32) * rate
                s = jnp.where(k_at <= pos * block + q_row, s, -2e30)
                old = again_top[0:1, :]
                new = jnp.maximum(old, jnp.max(s, axis=0, keepdims=True))
                p = jnp.exp2(s - new)
                fade = jnp.exp2(old - new)
                again_top[0:1, :] = new
                again_top[1:2, :] = again_top[1:2, :] * fade + jnp.sum(p, axis=0, keepdims=True)
                v = kv_all[core, zc, at, 1, b].T
                again_acc[...] = again_acc[...] * fade + jnp.dot(
                    v, p.astype(jnp.bfloat16), preferred_element_type=jnp.float32)
            return carry

        lax.fori_loop(0, 2 * RING * ROW, one, 0)
        put(t, again_top[1:2, :], again_acc[...], again_top[0:1, :])
        return carry

    @pl.when(jnp.max(worst) > 0)
    def _():
        lax.fori_loop(0, tiles, redo, 0)


def finish(places, order, rank, q_all, kv_all, acc, total, top, q_turned, marks):
    smem = pl.BlockSpec(memory_space=pltpu.SMEM)
    vmem = pl.BlockSpec(memory_space=pltpu.VMEM)
    tiles, width, lanes = acc.shape
    far = (RING - NEAR) * 2 * ROW * EACH * kv_all.shape[-2]
    return pl.pallas_call(
        finish_kernel,
        out_shape=(jax.ShapeDtypeStruct((tiles, lanes, width), jnp.bfloat16),
                   jax.ShapeDtypeStruct((tiles, 1, lanes), jnp.float32)),
        in_specs=[vmem, smem, smem, *[vmem] * 7],
        out_specs=(vmem, vmem),
        scratch_shapes=[
            pltpu.VMEM((far, width), jnp.bfloat16),
            pltpu.VMEM((far, width), jnp.bfloat16),
            pltpu.VMEM((far // width, width, width), jnp.bfloat16),
            [pltpu.VMEM((marks.shape[0], lanes), jnp.bfloat16)] * 2,
            pltpu.VMEM(acc.shape, jnp.float32),
            pltpu.VMEM(total.shape, jnp.float32),
            pltpu.VMEM((width, lanes), jnp.float32),
            pltpu.VMEM((8, lanes), jnp.float32),
        ],
        compiler_params=pltpu.CompilerParams(vmem_limit_bytes=28 * 1024 * 1024),
    )(places, order, rank, q_all, kv_all, acc, total, top, q_turned, marks)


def return_kernel(o_ref, lse_ref, o_all, lse_all, relay, o_send, o_recv, l_send, l_recv,
                  far_send, far_recv, on_send, on_recv, own_sem):
    x, z, c, y = place()
    steps, mates = row_mates(x, z, c, y)
    mate = dict(zip(steps, mates))
    greet(mates)
    keep = [pltpu.make_async_copy(o_ref.at[x, c], o_all.at[x, c], own_sem.at[0]),
            pltpu.make_async_copy(lse_ref.at[x, c], lse_all.at[x, c], own_sem.at[1])]
    copies, far = [], []
    for side, dx in ((0, 1), (1, 3)):
        for dc in range(2):
            far.append(remote(o_ref.at[(x + 2) % ROW, (c + dc) % 2, side], relay.at[side, dc],
                              far_send.at[side, dc], far_recv.at[side, dc], mate[dx, 0]))
            far[-1].start()
    for n, (dx, dc) in enumerate(steps):
        to_x, to_c = (x + dx) % ROW, (c + dc) % 2
        copies.append(remote(lse_ref.at[to_x, to_c], lse_all.at[x, c], l_send.at[n], l_recv.at[n], mates[n]))
        copies[-1].start()
        if dx != 2:
            copies.append(remote(o_ref.at[to_x, to_c], o_all.at[x, c], o_send.at[n], o_recv.at[n], mates[n]))
            copies[-1].start()
    for copy in keep:
        copy.start()
    for k, (side, dx) in enumerate(((0, 1), (1, 3))):
        for dc in range(2):
            far[2 * k + dc].wait()
            copies.append(remote(relay.at[side, dc], o_all.at[(x + ROW - dx) % ROW, c, side],
                                 on_send.at[side, dc], on_recv.at[side, dc], mate[dx, dc]))
            copies[-1].start()
    for copy in [*keep, *copies]:
        copy.wait()


def send_back(o, lse):
    sem = pltpu.SemaphoreType.DMA
    vmem = pl.BlockSpec(memory_space=pltpu.VMEM)
    n = 2 * ROW - 1
    return pl.pallas_call(
        return_kernel,
        out_shape=(jax.ShapeDtypeStruct(o.shape, o.dtype), jax.ShapeDtypeStruct(lse.shape, lse.dtype)),
        in_specs=[vmem, vmem],
        out_specs=(vmem, vmem),
        scratch_shapes=[pltpu.VMEM((2, 2, *o.shape[-2:]), o.dtype),
                        sem((n,)), sem((n,)), sem((n,)), sem((n,)),
                        sem((2, 2)), sem((2, 2)), sem((2, 2)), sem((2, 2)), sem((2,))],
        compiler_params=pltpu.CompilerParams(
            collective_id=1, has_side_effects=True, vmem_limit_bytes=32 * 1024 * 1024),
        cost_estimate=pl.CostEstimate(flops=0, bytes_accessed=20_000_000, transcendentals=0),
    )(o, lse)


def body(stored_query_rows, stored_key_rows, stored_value_rows, span_order):
    rows, heads, width = stored_query_rows.shape
    span = rows // EACH
    q = stored_query_rows.reshape(EACH, span, 2, 2, 2, width).transpose(2, 3, 0, 4, 1, 5)
    q = q.reshape(2, 2, EACH, 2 * span, width)
    kv = jnp.stack([stored_key_rows, stored_value_rows])
    kv = kv.reshape(2, EACH, 2, span // 2, 2, width).transpose(4, 2, 0, 1, 3, 5)
    kv = kv.reshape(4, 2, EACH, span // 2, width)
    places = span_order.reshape(RING // 2, 2, ROW, 2, EACH).transpose(0, 3, 1, 2, 4)
    flat = places.reshape(-1)
    places = jnp.broadcast_to(places.reshape(RING, 2 * ROW * EACH, 1), (RING, 2 * ROW * EACH, 2 * span))
    away = (jnp.arange(flat.shape[0]) // (2 * ROW * EACH) - place()[1] + RING + NEAR // 2) % RING >= NEAR
    rank = jnp.sum((away[None, :] & (flat[None, :] < flat[:, None])).astype(jnp.int32), axis=1)
    o, lse = finish(places, span_order, rank, *attend(places, q, kv))

    o, lse = send_back(o.reshape(ROW, 2, EACH, 2 * span, width), lse.reshape(ROW, 2, EACH, 1, 2 * span))
    o = o.reshape(2, 2, 2, EACH, 2, span, width)
    lse = lse.reshape(2, 2, 2, EACH, 2, span)
    top = jnp.max(lse, axis=0)
    weights = jnp.exp2(lse - top)
    share = weights / jnp.sum(weights, axis=0)
    result = jnp.sum(o.astype(jnp.float32) * share[..., None], axis=0).astype(jnp.bfloat16)
    return result.transpose(2, 4, 0, 1, 3, 5).reshape(rows, heads, width)


def solution(mesh):
    placed = (
        P(("outer", "inner"), "head", None),
        P(("outer", "inner"), "head", None),
        P(("outer", "inner"), "head", None),
        P(),
    )
    return jax.shard_map(
        body,
        mesh=mesh,
        in_specs=placed,
        out_specs=P(("outer", "inner"), "head", None),
        check_vma=False,
    )
```

```python
import math

import jax
import jax.numpy as jnp
from jax import lax
from jax.experimental import pallas as pl
from jax.experimental.pallas import tpu as pltpu
from jax.sharding import PartitionSpec as P

ROW = 4
RING = 8
EACH = 2
NEAR = 3
MESH = pl.DeviceIdType.MESH
NEVER = 2.0**20


def place():
    outer, inner = lax.axis_index("outer"), lax.axis_index("inner")
    return inner // 2, outer // 2 * 2 + inner % 2, outer % 2, lax.axis_index("head")


def device(x, z, c, y):
    return (z // 2 * 2 + c, x * 2 + z % 2, y)


def greet(peers):
    barrier = pltpu.get_barrier_semaphore()
    for peer in peers:
        pl.semaphore_signal(barrier, inc=1, device_id=peer, device_id_type=MESH)
    pl.semaphore_wait(barrier, len(peers))


def row_mates(x, z, c, y):
    steps = [(dx, dc) for dx in range(ROW) for dc in range(2) if (dx, dc) != (0, 0)]
    return steps, [device((x + dx) % ROW, z, (c + dc) % 2, y) for dx, dc in steps]


def remote(src, dst, send, recv, to):
    return pltpu.make_async_remote_copy(
        src_ref=src, dst_ref=dst, send_sem=send, recv_sem=recv, device_id=to, device_id_type=MESH)


def attend_kernel(place_ref, q_ref, kv_ref, q_all, kv_all, acc, total, top, q_turned, marks,
                  v_turned, p_bufs, relay,
                  q_send, q_recv, far_send, far_recv, on_send, on_recv, x_send, x_recv,
                  up_send, up_recv, down_send, down_recv, core_send, core_recv, own_sem):
    x, z, c, y = place()
    steps, mates = row_mates(x, z, c, y)
    mate = dict(zip(steps, mates))
    above, below = device(x, (z + 1) % RING, c, y), device(x, (z + RING - 1) % RING, c, y)
    partner = mate[0, 1]
    greet([*mates, above, below])
    piece, width = kv_ref.shape[-2:]
    block = 2 * piece
    lanes = q_ref.shape[-2]
    tiles = 2 * ROW * EACH
    window = 2 * ROW * EACH * piece
    rate = math.log2(math.e) / math.sqrt(width)
    half = x // 2
    role = x % 2 * 2 + x // 2
    mine = kv_ref.at[role]

    def slot_of(off, j):
        return kv_all.at[c, (z + off + RING) % RING, (x + j) % ROW]

    def pass_up(t, j, src):
        remote(src, slot_of(-t, j), up_send.at[t, j], up_recv.at[t, j], above).start()

    def pass_down(t, j, src):
        remote(src, slot_of(t, j), down_send.at[t, j], down_recv.at[t, j], below).start()

    def to_partner(off, j, src):
        r = (off + RING) % RING
        remote(src, slot_of(off, j), core_send.at[r, j], core_recv.at[r, j], partner).start()

    def arrived(dst, recv):
        remote(dst, dst, x_send.at[1], recv, partner).wait_recv()

    def gone(src, send):
        remote(src, src, send, x_recv.at[1], partner).wait_send()

    pass_up(0, 0, mine)
    pass_down(0, 0, mine)
    for d in (1, 3, 2):
        to = (x + d) % ROW
        remote(kv_ref.at[to % 2 * 2 + to // 2], kv_all.at[c, z, x], x_send.at[d], x_recv.at[d],
               device(to, z, c, y)).start()
    to_partner(0, 0, mine)
    keep_kv = pltpu.make_async_copy(mine, kv_all.at[c, z, x], own_sem.at[0])
    keep_q = pltpu.make_async_copy(q_ref.at[x % 2, c], q_all.at[x, c], own_sem.at[1])
    keep_kv.start()
    keep_q.start()
    for n, (dx, dc) in enumerate(steps):
        if dx != 2:
            remote(q_ref.at[(x + dx) % 2, (c + dc) % 2], q_all.at[x, c], q_send.at[n], q_recv.at[n],
                   mates[n]).start()
    for side, dx in ((0, 1), (1, 3)):
        for dc in range(2):
            remote(q_ref.at[x % 2, (c + dc) % 2, side], relay.at[side, dc], far_send.at[side, dc],
                   far_recv.at[side, dc], mate[dx, 0]).start()

    k_row = lax.broadcasted_iota(jnp.int32, (window, width), 0)
    column = lax.broadcasted_iota(jnp.int32, (window, width), 1)
    marks[...] = jnp.where((column == k_row // piece) | (column == tiles), 1.0, 0.0).astype(marks.dtype)
    q_turned[:, width + tiles:, :] = jnp.zeros((tiles, width - tiles, lanes), q_turned.dtype)

    for j in (1, 3, 2):
        slot = slot_of(0, j)
        arrived(slot, x_recv.at[ROW - j])
        pass_up(0, j, slot)
        pass_down(0, j, slot)
        to_partner(0, j, slot)
    keep_kv.wait()
    keep_q.wait()

    def forward():
        for side, dx in ((0, 1), (1, 3)):
            for dc in range(2):
                arrived(relay.at[side, dc], far_recv.at[side, dc])
                remote(relay.at[side, dc], q_all.at[(x + ROW - dx) % ROW, c, side], on_send.at[side, dc],
                       on_recv.at[side, dc], mate[dx, dc]).start()

    def ready(zc):
        r = (zc - z + RING) % RING
        for j in range(ROW):
            arrived(kv_all.at[1 - c, zc, (x + j) % ROW], core_recv.at[r, j])
        for core in range(2):
            for at in range(ROW):
                v = kv_all[core, zc, at, 1].reshape(EACH * piece, width)
                v_turned[(core * RING + zc) * ROW + at] = v.T

    ready(z)

    own_k = lax.broadcasted_iota(jnp.int32, (piece, lanes), 0) + half * piece
    own_allowed = own_k <= lax.broadcasted_iota(jnp.int32, (piece, lanes), 1) % block

    def take(at, core):
        for b in range(EACH):
            t = (at * 2 + core) * EACH + b
            q = q_all[at, core, b].T
            q_turned[t, :width, :] = q
            s = jnp.dot(kv_all[core, z, at, 0, b], q, preferred_element_type=jnp.float32)
            ref = jnp.max(s, axis=0, keepdims=True).astype(jnp.bfloat16).astype(jnp.float32)
            top[t] = ref
            first = lax.broadcasted_iota(jnp.int32, (tiles, lanes), 0) == 0
            q_turned[t, width + tiles:width + 2 * tiles, :] = jnp.where(first, -ref, 0.0).astype(q_turned.dtype)
            p = jnp.where(own_allowed, jnp.exp2((s - ref) * rate), 0.0)
            total[t] = jnp.sum(p.reshape(piece // 8, 8, lanes), axis=0)
            v = v_turned[(core * RING + z) * ROW + at]
            acc[t] = jnp.dot(v[:, b * piece:(b + 1) * piece], p.astype(jnp.bfloat16), preferred_element_type=jnp.float32)

    take(x, c)
    arrived(q_all.at[x, 1 - c], q_recv.at[steps.index((0, 1))])
    take(x, 1 - c)

    def await_queries(dx):
        for core in range(2):
            if dx == 2:
                for side in range(2):
                    dc = (core + c) % 2
                    arrived(q_all.at[(x + 2) % ROW, core, side], on_recv.at[side, dc])
            else:
                dc = (core + c) % 2
                arrived(q_all.at[(x + ROW - dx) % ROW, core], q_recv.at[steps.index((dx, 0)) + dc])

    def row_at(n):
        off = jnp.where(n % 2 == 1, -((n + 1) // 2), n // 2)
        return off, (z + off + RING) % RING

    def weigh(t, zc, buf):
        own = (t // EACH % 2 * ROW + t // (2 * EACH)) * EACH + t % EACH
        before = place_ref[zc] < place_ref[z, pl.ds(own, 1), :]
        q_turned[t, width:width + tiles, :] = jnp.where(before, 0.0, -NEVER).astype(q_turned.dtype)
        k = [kv_all[core, zc, at, 0].reshape(EACH * piece, width) for core in range(2) for at in range(ROW)]
        keys = jnp.concatenate([jnp.concatenate(k, axis=0), marks[...]], axis=1)
        s = jnp.dot(keys, q_turned[t], preferred_element_type=jnp.float32)
        p = jnp.exp2(s * rate)
        total[t] += jnp.sum(p.reshape(window // 8, 8, lanes), axis=0)
        p_bufs[buf][...] = p.astype(jnp.bfloat16)

    def absorb(t, zc, buf):
        v = [v_turned[(core * RING + zc) * ROW + at] for core in range(2) for at in range(ROW)]
        acc[t] += jnp.dot(jnp.concatenate(v, axis=1), p_bufs[buf][...], preferred_element_type=jnp.float32)

    def rise(t, j):
        slot = slot_of(-t, j)
        arrived(slot, up_recv.at[t - 1, j])

        @pl.when((t < 3) | ((t == 3) & (j < 2)))
        def _():
            pass_up(t, j, slot)

        to_partner(-t, j, slot)

    def fall(t, j):
        slot = slot_of(t, j)
        arrived(slot, down_recv.at[t - 1, j])

        @pl.when((t < 3) | ((t == 3) & (j >= 2)))
        def _():
            pass_down(t, j, slot)

        to_partner(t, j, slot)

    for j in (0, 1, 3, 2):
        rise(1, j)
        fall(1, j)

    per_turn = 2 * EACH
    turns = ROW * NEAR

    def plan(m):
        g = m // NEAR
        chip = (x + jnp.where(g == 1, 3, jnp.where(g == 2, 1, jnp.where(g == 3, 2, 0)))) % ROW
        return chip, chip * per_turn, row_at(m % NEAR)[1]

    def hop(event):
        t, j = event // ROW + 2, event % ROW
        j = jnp.where(j == 2, 3, jnp.where(j == 3, 2, j))
        rise(t, j)
        fall(t, j)

    def turn(m, carry):
        _, base, zc = plan(m)
        chip, next_base, next_zc = plan(m + 1)

        @pl.when(m < NEAR - 1)
        def _():
            ready(next_zc)

        @pl.when((m >= NEAR - 1) & (m <= 3 * NEAR - 1))
        def _():
            hop(m - NEAR + 1 + jnp.where(m > 2 * NEAR, 1, 0))

        @pl.when(m == 2 * NEAR)
        def _():
            hop(m - NEAR + 2)

        @pl.when(m == turns - 2)
        def _():
            rise(RING // 2, 0)
            fall(RING // 2, 3)

        for g, dx in ((1, 1), (2, 3), (3, 2)):
            @pl.when(m == NEAR * g - 1)
            def _(dx=dx):
                await_queries(dx)

        @pl.when(m == NEAR + 1)
        def _():
            forward()

        @pl.when((m == NEAR - 1) | (m == 2 * NEAR - 1) | (m == 3 * NEAR - 1))
        def _():
            take(chip, 0)
            take(chip, 1)

        for u in range(per_turn):
            done = u == per_turn - 1
            weigh(next_base if done else base + u + 1, next_zc if done else zc, 1 - u % 2)
            absorb(base + u, zc, u % 2)
        return carry

    weigh(x * per_turn, z, 0)
    lax.fori_loop(0, turns - 1, turn, 0)
    rise(RING // 2, 1)
    fall(RING // 2, 2)
    _, last_base, last_zc = plan(turns - 1)
    for u in range(per_turn):
        if u < per_turn - 1:
            weigh(last_base + u + 1, last_zc, 1 - u % 2)
        absorb(last_base + u, last_zc, u % 2)
    for r in range(2, RING - 1):
        for j in range(ROW):
            arrived(kv_all.at[1 - c, (z + r) % RING, (x + j) % ROW], core_recv.at[r, j])

    for j in range(ROW):
        for t in range(RING // 2):
            if t < 3 or j < 2:
                gone(slot_of(0, j), up_send.at[t, j])
            if t < 3 or j >= 2:
                gone(slot_of(0, j), down_send.at[t, j])
        for r in range(RING):
            gone(slot_of(0, j), core_send.at[r, j])
        if j:
            gone(slot_of(0, j), x_send.at[j])
    for side in range(2):
        for dc in range(2):
            gone(relay.at[side, dc], far_send.at[side, dc])
            gone(relay.at[side, dc], on_send.at[side, dc])
    for n, (dx, dc) in enumerate(steps):
        if dx != 2:
            gone(q_all.at[x, c], q_send.at[n])


def attend(places, q, kv):
    sem = pltpu.SemaphoreType.DMA
    half_ring = RING // 2
    vmem = pl.BlockSpec(memory_space=pltpu.VMEM)
    lanes, width = q.shape[-2:]
    piece = kv.shape[-2]
    tiles = 2 * ROW * EACH
    window = tiles * piece
    return pl.pallas_call(
        attend_kernel,
        out_shape=(jax.ShapeDtypeStruct((ROW, 2, *q.shape[2:]), q.dtype),
                   jax.ShapeDtypeStruct((2, RING, ROW, *kv.shape[1:]), kv.dtype),
                   jax.ShapeDtypeStruct((tiles, width, lanes), jnp.float32),
                   jax.ShapeDtypeStruct((tiles, 8, lanes), jnp.float32),
                   jax.ShapeDtypeStruct((tiles, 1, lanes), jnp.float32),
                   jax.ShapeDtypeStruct((tiles, 2 * width, lanes), jnp.bfloat16),
                   jax.ShapeDtypeStruct((window, width), jnp.bfloat16)),
        in_specs=[vmem] * 3,
        out_specs=(vmem,) * 7,
        scratch_shapes=[
            pltpu.VMEM((2 * RING * ROW, width, width), jnp.bfloat16),
            [pltpu.VMEM((window, lanes), jnp.bfloat16)] * 2,
            pltpu.VMEM((2, 2, lanes, width), jnp.bfloat16),
            sem((2 * ROW - 1,)), sem((2 * ROW - 1,)), sem((2, 2)), sem((2, 2)), sem((2, 2)), sem((2, 2)),
            sem((ROW,)), sem((ROW,)),
            sem((half_ring, ROW)), sem((half_ring, ROW)), sem((half_ring, ROW)), sem((half_ring, ROW)),
            sem((RING, ROW)), sem((RING, ROW)), sem((2,)),
        ],
        compiler_params=pltpu.CompilerParams(
            collective_id=0, has_side_effects=True, vmem_limit_bytes=32 * 1024 * 1024),
        cost_estimate=pl.CostEstimate(flops=10**10, bytes_accessed=20_000_000, transcendentals=0),
    )(places, q, kv)


def finish_kernel(place_ref, order, rank, q_all, kv_all, acc, total, top, q_turned, marks, o_ref, lse_ref,
                  k_sorted, v_sorted, v_turned, p_bufs, far_acc, far_total, again_acc, again_top):
    x, z, _, _ = place()
    half = x // 2
    tiles, _, lanes = acc.shape
    piece, width = kv_all.shape[-2:]
    block = 2 * piece
    rate = math.log2(math.e) / math.sqrt(width)
    q_row = lax.broadcasted_iota(jnp.int32, (1, lanes), 1) % block

    def stored(zc, core, at, b):
        return order[((zc // 2 * 2 + core) * RING + at * 2 + zc % 2) * EACH + b]

    def put(t, weight, sums, reference):
        some = weight > 0
        weight = jnp.where(some, weight, 1.0)
        o_ref[t] = (sums * (1.0 / weight)).T.astype(jnp.bfloat16)
        lse_ref[t] = jnp.where(some, reference + jnp.log2(weight), -1e30)

    window = marks.shape[0]
    per_window = window // piece

    def sort(i, carry):
        n, g = i // (2 * ROW), i % (2 * ROW)
        off = jnp.where(n % 2 == 1, (n + 3) // 2, -((n + 4) // 2))
        zc = (z + off + RING) % RING
        core, at_x = g // ROW, g % ROW
        for b in range(EACH):
            at = pl.multiple_of(rank[((zc * 2 + core) * ROW + at_x) * EACH + b] * piece, piece)
            k_sorted[pl.ds(at, piece), :] = kv_all[core, zc, at_x, 0, b]
            v_sorted[pl.ds(at, piece), :] = kv_all[core, zc, at_x, 1, b]
        return carry

    lax.fori_loop(0, (RING - NEAR) * 2 * ROW, sort, 0, unroll=4)

    def turn(g, carry):
        at = pl.multiple_of(g * width, width)
        v_turned[g] = v_sorted[pl.ds(at, width), :].T
        return carry

    lax.fori_loop(0, v_turned.shape[0], turn, 0, unroll=8)

    def own_row(t):
        return (t // EACH % 2 * ROW + t // (2 * EACH)) * EACH + t % EACH

    def count_of(t):
        held = rank[z * tiles + own_row(jnp.minimum(t, tiles - 1))]
        return jnp.where(t < tiles, held, 0)

    def clear(t, items):
        far_acc[t] = jnp.zeros(far_acc.shape[1:], jnp.float32)
        far_total[t] = jnp.zeros(far_total.shape[1:], jnp.float32)
        return items + jnp.maximum((count_of(t) + per_window - 1) // per_window, 1)

    items = lax.fori_loop(0, tiles, clear, 0)
    block_row = lax.broadcasted_iota(jnp.int32, (tiles, lanes), 0)

    def weigh(t, w, buf):
        count, t = count_of(t), jnp.minimum(t, tiles - 1)
        at = pl.multiple_of(w * window, window)
        mask = jnp.where(block_row < count - w * per_window, 0.0, -NEVER).astype(q_turned.dtype)
        right = jnp.concatenate([q_turned[t, :width, :], mask, q_turned[t, width + tiles:, :]], axis=0)
        keys = jnp.concatenate([k_sorted[pl.ds(at, window), :], marks[...]], axis=1)
        p = jnp.exp2(jnp.dot(keys, right, preferred_element_type=jnp.float32) * rate)
        far_total[t] += jnp.sum(p.reshape(window // 8, 8, lanes), axis=0)
        p_bufs[buf][...] = p.astype(jnp.bfloat16)

    def absorb(t, w, buf):
        t = jnp.minimum(t, tiles - 1)
        v = [v_turned[w * (window // width) + i] for i in range(window // width)]
        far_acc[t] += jnp.dot(jnp.concatenate(v, axis=1), p_bufs[buf][...], preferred_element_type=jnp.float32)

    unroll = 4

    def step(i, at):
        t, w = at
        for u in range(unroll):
            last = (w + 1) * per_window >= count_of(t)
            next_t, next_w = jnp.where(last, t + 1, t), jnp.where(last, 0, w + 1)
            weigh(next_t, next_w, 1 - u % 2)
            absorb(t, w, u % 2)
            t, w = next_t, next_w
        return t, w

    weigh(jnp.int32(0), jnp.int32(0), 0)
    lax.fori_loop(0, (items + unroll - 1) // unroll, step, (jnp.int32(0), jnp.int32(0)))

    worst = jnp.zeros((1, lanes), jnp.float32)
    for t in range(tiles):
        weight = jnp.sum(total[t] + far_total[t], axis=0, keepdims=True)
        own = own_row(t)
        no_key = (place_ref[z, own:own + 1, :] == 0) & (q_row < half * piece)
        fits = ((weight > 2.0**-60) & (weight < 2.0**80)) | no_key
        worst = jnp.maximum(worst, jnp.where(fits, 0.0, 1.0))
        put(t, weight, acc[t] + far_acc[t], top[t] * rate)

    def redo(t, carry):
        at_q, core_q, b_q = t // (2 * EACH), t // EACH % 2, t % EACH
        pos = stored(z, core_q, at_q, b_q)
        q = q_all[at_q, core_q, b_q].T
        again_acc[...] = jnp.zeros_like(again_acc)
        again_top[0:1, :] = jnp.full((1, lanes), -1e30, jnp.float32)
        again_top[1:2, :] = jnp.zeros((1, lanes), jnp.float32)

        def one(g, carry):
            core, zc, at = g // (RING * ROW), g // ROW % RING, g % ROW
            for b in range(EACH):
                kp = stored(zc, core, at, b)
                k_at = lax.broadcasted_iota(jnp.int32, (piece, lanes), 0) + half * piece + kp * block
                s = jnp.dot(kv_all[core, zc, at, 0, b], q, preferred_element_type=jnp.float32) * rate
                s = jnp.where(k_at <= pos * block + q_row, s, -2e30)
                old = again_top[0:1, :]
                new = jnp.maximum(old, jnp.max(s, axis=0, keepdims=True))
                p = jnp.exp2(s - new)
                fade = jnp.exp2(old - new)
                again_top[0:1, :] = new
                again_top[1:2, :] = again_top[1:2, :] * fade + jnp.sum(p, axis=0, keepdims=True)
                v = kv_all[core, zc, at, 1, b].T
                again_acc[...] = again_acc[...] * fade + jnp.dot(
                    v, p.astype(jnp.bfloat16), preferred_element_type=jnp.float32)
            return carry

        lax.fori_loop(0, 2 * RING * ROW, one, 0)
        put(t, again_top[1:2, :], again_acc[...], again_top[0:1, :])
        return carry

    @pl.when(jnp.max(worst) > 0)
    def _():
        lax.fori_loop(0, tiles, redo, 0)


def finish(places, order, rank, q_all, kv_all, acc, total, top, q_turned, marks):
    smem = pl.BlockSpec(memory_space=pltpu.SMEM)
    vmem = pl.BlockSpec(memory_space=pltpu.VMEM)
    tiles, width, lanes = acc.shape
    far = (RING - NEAR) * 2 * ROW * EACH * kv_all.shape[-2]
    return pl.pallas_call(
        finish_kernel,
        out_shape=(jax.ShapeDtypeStruct((tiles, lanes, width), jnp.bfloat16),
                   jax.ShapeDtypeStruct((tiles, 1, lanes), jnp.float32)),
        in_specs=[vmem, smem, smem, *[vmem] * 7],
        out_specs=(vmem, vmem),
        scratch_shapes=[
            pltpu.VMEM((far, width), jnp.bfloat16),
            pltpu.VMEM((far, width), jnp.bfloat16),
            pltpu.VMEM((far // width, width, width), jnp.bfloat16),
            [pltpu.VMEM((marks.shape[0], lanes), jnp.bfloat16)] * 2,
            pltpu.VMEM(acc.shape, jnp.float32),
            pltpu.VMEM(total.shape, jnp.float32),
            pltpu.VMEM((width, lanes), jnp.float32),
            pltpu.VMEM((8, lanes), jnp.float32),
        ],
        compiler_params=pltpu.CompilerParams(vmem_limit_bytes=28 * 1024 * 1024),
    )(places, order, rank, q_all, kv_all, acc, total, top, q_turned, marks)


def return_kernel(o_ref, lse_ref, o_all, lse_all, relay, o_send, o_recv, l_send, l_recv,
                  far_send, far_recv, on_send, on_recv, own_sem):
    x, z, c, y = place()
    steps, mates = row_mates(x, z, c, y)
    mate = dict(zip(steps, mates))
    greet(mates)
    keep = [pltpu.make_async_copy(o_ref.at[x, c], o_all.at[x, c], own_sem.at[0]),
            pltpu.make_async_copy(lse_ref.at[x, c], lse_all.at[x, c], own_sem.at[1])]
    copies, far = [], []
    for side, dx in ((0, 1), (1, 3)):
        for dc in range(2):
            far.append(remote(o_ref.at[(x + 2) % ROW, (c + dc) % 2, side], relay.at[side, dc],
                              far_send.at[side, dc], far_recv.at[side, dc], mate[dx, 0]))
            far[-1].start()
    for n, (dx, dc) in enumerate(steps):
        to_x, to_c = (x + dx) % ROW, (c + dc) % 2
        copies.append(remote(lse_ref.at[to_x, to_c], lse_all.at[x, c], l_send.at[n], l_recv.at[n], mates[n]))
        copies[-1].start()
        if dx != 2:
            copies.append(remote(o_ref.at[to_x, to_c], o_all.at[x, c], o_send.at[n], o_recv.at[n], mates[n]))
            copies[-1].start()
    for copy in keep:
        copy.start()
    for k, (side, dx) in enumerate(((0, 1), (1, 3))):
        for dc in range(2):
            far[2 * k + dc].wait()
            copies.append(remote(relay.at[side, dc], o_all.at[(x + ROW - dx) % ROW, c, side],
                                 on_send.at[side, dc], on_recv.at[side, dc], mate[dx, dc]))
            copies[-1].start()
    for copy in [*keep, *copies]:
        copy.wait()


def send_back(o, lse):
    sem = pltpu.SemaphoreType.DMA
    vmem = pl.BlockSpec(memory_space=pltpu.VMEM)
    n = 2 * ROW - 1
    return pl.pallas_call(
        return_kernel,
        out_shape=(jax.ShapeDtypeStruct(o.shape, o.dtype), jax.ShapeDtypeStruct(lse.shape, lse.dtype)),
        in_specs=[vmem, vmem],
        out_specs=(vmem, vmem),
        scratch_shapes=[pltpu.VMEM((2, 2, *o.shape[-2:]), o.dtype),
                        sem((n,)), sem((n,)), sem((n,)), sem((n,)),
                        sem((2, 2)), sem((2, 2)), sem((2, 2)), sem((2, 2)), sem((2,))],
        compiler_params=pltpu.CompilerParams(
            collective_id=1, has_side_effects=True, vmem_limit_bytes=32 * 1024 * 1024),
        cost_estimate=pl.CostEstimate(flops=0, bytes_accessed=20_000_000, transcendentals=0),
    )(o, lse)


def body(stored_query_rows, stored_key_rows, stored_value_rows, span_order):
    rows, heads, width = stored_query_rows.shape
    span = rows // EACH
    q = stored_query_rows.reshape(EACH, span, 2, 2, 2, width).transpose(2, 3, 0, 4, 1, 5)
    q = q.reshape(2, 2, EACH, 2 * span, width)
    kv = jnp.stack([stored_key_rows, stored_value_rows])
    kv = kv.reshape(2, EACH, 2, span // 2, 2, width).transpose(4, 2, 0, 1, 3, 5)
    kv = kv.reshape(4, 2, EACH, span // 2, width)
    places = span_order.astype(jnp.float32).reshape(RING // 2, 2, ROW, 2, EACH).transpose(0, 3, 1, 2, 4)
    flat = places.reshape(-1)
    places = jnp.broadcast_to(places.reshape(RING, 2 * ROW * EACH, 1), (RING, 2 * ROW * EACH, 2 * span))
    away = (jnp.arange(flat.shape[0]) // (2 * ROW * EACH) - place()[1] + RING + NEAR // 2) % RING >= NEAR
    rank = jnp.sum((away[None, :] & (flat[None, :] < flat[:, None])).astype(jnp.int32), axis=1)
    o, lse = finish(places, span_order, rank, *attend(places, q, kv))

    o, lse = send_back(o.reshape(ROW, 2, EACH, 2 * span, width), lse.reshape(ROW, 2, EACH, 1, 2 * span))
    o = o.reshape(2, 2, 2, EACH, 2, span, width)
    lse = lse.reshape(2, 2, 2, EACH, 2, span)
    top = jnp.max(lse, axis=0)
    weights = jnp.exp2(lse - top)
    share = weights / jnp.sum(weights, axis=0)
    result = jnp.sum(o.astype(jnp.float32) * share[..., None], axis=0).astype(jnp.bfloat16)
    return result.transpose(2, 4, 0, 1, 3, 5).reshape(rows, heads, width)


def solution(mesh):
    placed = (
        P(("outer", "inner"), "head", None),
        P(("outer", "inner"), "head", None),
        P(("outer", "inner"), "head", None),
        P(),
    )
    return jax.shard_map(
        body,
        mesh=mesh,
        in_specs=placed,
        out_specs=P(("outer", "inner"), "head", None),
        check_vma=False,
    )
```

```python
import math

import jax
import jax.numpy as jnp
from jax import lax
from jax.experimental import pallas as pl
from jax.experimental.pallas import tpu as pltpu
from jax.sharding import PartitionSpec as P

ROW = 4
RING = 8
EACH = 2
NEAR = 3
MESH = pl.DeviceIdType.MESH
NEVER = 2.0**20


def place():
    outer, inner = lax.axis_index("outer"), lax.axis_index("inner")
    return inner // 2, outer // 2 * 2 + inner % 2, outer % 2, lax.axis_index("head")


def device(x, z, c, y):
    return (z // 2 * 2 + c, x * 2 + z % 2, y)


def stored(z, core, x, b):
    return ((z // 2 * 2 + core) * RING + x * 2 + z % 2) * EACH + b


def greet(peers):
    barrier = pltpu.get_barrier_semaphore()
    for peer in peers:
        pl.semaphore_signal(barrier, inc=1, device_id=peer, device_id_type=MESH)
    pl.semaphore_wait(barrier, len(peers))


def row_mates(x, z, c, y):
    steps = [(dx, dc) for dx in range(ROW) for dc in range(2) if (dx, dc) != (0, 0)]
    return steps, [device((x + dx) % ROW, z, (c + dc) % 2, y) for dx, dc in steps]


def remote(src, dst, send, recv, to):
    return pltpu.make_async_remote_copy(
        src_ref=src, dst_ref=dst, send_sem=send, recv_sem=recv, device_id=to, device_id_type=MESH)


def attend_kernel(order, q_ref, kv_ref, q_all, kv_all, acc, total, top, q_turned, marks,
                  place_ref, v_turned, p_bufs, relay,
                  q_send, q_recv, far_send, far_recv, on_send, on_recv, x_send, x_recv,
                  up_send, up_recv, down_send, down_recv, core_send, core_recv, own_sem):
    x, z, c, y = place()
    steps, mates = row_mates(x, z, c, y)
    mate = dict(zip(steps, mates))
    above, below = device(x, (z + 1) % RING, c, y), device(x, (z + RING - 1) % RING, c, y)
    partner = mate[0, 1]
    greet([*mates, above, below])
    piece, width = kv_ref.shape[-2:]
    block = 2 * piece
    lanes = q_ref.shape[-2]
    tiles = 2 * ROW * EACH
    window = 2 * ROW * EACH * piece
    rate = math.log2(math.e) / math.sqrt(width)
    half = x // 2
    role = x % 2 * 2 + x // 2
    mine = kv_ref.at[role]

    def slot_of(off, j):
        return kv_all.at[c, (z + off + RING) % RING, (x + j) % ROW]

    def pass_up(t, j, src):
        remote(src, slot_of(-t, j), up_send.at[t, j], up_recv.at[t, j], above).start()

    def pass_down(t, j, src):
        remote(src, slot_of(t, j), down_send.at[t, j], down_recv.at[t, j], below).start()

    def to_partner(off, j, src):
        r = (off + RING) % RING
        remote(src, slot_of(off, j), core_send.at[r, j], core_recv.at[r, j], partner).start()

    def arrived(dst, recv):
        remote(dst, dst, x_send.at[1], recv, partner).wait_recv()

    def gone(src, send):
        remote(src, src, send, x_recv.at[1], partner).wait_send()

    pass_up(0, 0, mine)
    pass_down(0, 0, mine)
    for d in (1, 3, 2):
        to = (x + d) % ROW
        remote(kv_ref.at[to % 2 * 2 + to // 2], kv_all.at[c, z, x], x_send.at[d], x_recv.at[d],
               device(to, z, c, y)).start()
    to_partner(0, 0, mine)
    keep_kv = pltpu.make_async_copy(mine, kv_all.at[c, z, x], own_sem.at[0])
    keep_q = pltpu.make_async_copy(q_ref.at[x % 2, c], q_all.at[x, c], own_sem.at[1])
    keep_kv.start()
    keep_q.start()
    for n, (dx, dc) in enumerate(steps):
        if dx != 2:
            remote(q_ref.at[(x + dx) % 2, (c + dc) % 2], q_all.at[x, c], q_send.at[n], q_recv.at[n],
                   mates[n]).start()
    for side, dx in ((0, 1), (1, 3)):
        for dc in range(2):
            remote(q_ref.at[x % 2, (c + dc) % 2, side], relay.at[side, dc], far_send.at[side, dc],
                   far_recv.at[side, dc], mate[dx, 0]).start()

    def spread(i, carry):
        zc, row = i // tiles, i % tiles
        held = order[stored(zc, row // (ROW * EACH), row // EACH % ROW, row % EACH)]
        place_ref[zc, pl.ds(row, 1), :] = jnp.full((1, lanes), held, jnp.int32)
        return carry

    lax.fori_loop(0, RING * tiles, spread, 0, unroll=4)

    k_row = lax.broadcasted_iota(jnp.int32, (window, width), 0)
    column = lax.broadcasted_iota(jnp.int32, (window, width), 1)
    marks[...] = jnp.where((column == k_row // piece) | (column == tiles), 1.0, 0.0).astype(marks.dtype)
    q_turned[:, width + tiles:, :] = jnp.zeros((tiles, width - tiles, lanes), q_turned.dtype)

    for j in (1, 3, 2):
        slot = slot_of(0, j)
        arrived(slot, x_recv.at[ROW - j])
        pass_up(0, j, slot)
        pass_down(0, j, slot)
        to_partner(0, j, slot)
    keep_kv.wait()
    keep_q.wait()

    def forward():
        for side, dx in ((0, 1), (1, 3)):
            for dc in range(2):
                arrived(relay.at[side, dc], far_recv.at[side, dc])
                remote(relay.at[side, dc], q_all.at[(x + ROW - dx) % ROW, c, side], on_send.at[side, dc],
                       on_recv.at[side, dc], mate[dx, dc]).start()

    def ready(zc):
        r = (zc - z + RING) % RING
        for j in range(ROW):
            arrived(kv_all.at[1 - c, zc, (x + j) % ROW], core_recv.at[r, j])
        for core in range(2):
            for at in range(ROW):
                v = kv_all[core, zc, at, 1].reshape(EACH * piece, width)
                v_turned[(core * RING + zc) * ROW + at] = v.T

    ready(z)

    own_k = lax.broadcasted_iota(jnp.int32, (piece, lanes), 0) + half * piece
    own_allowed = own_k <= lax.broadcasted_iota(jnp.int32, (piece, lanes), 1) % block

    def take(at, core):
        for b in range(EACH):
            t = (at * 2 + core) * EACH + b
            q = q_all[at, core, b].T
            q_turned[t, :width, :] = q
            s = jnp.dot(kv_all[core, z, at, 0, b], q, preferred_element_type=jnp.float32)
            ref = jnp.max(s, axis=0, keepdims=True).astype(jnp.bfloat16).astype(jnp.float32)
            top[t] = ref
            first = lax.broadcasted_iota(jnp.int32, (tiles, lanes), 0) == 0
            q_turned[t, width + tiles:width + 2 * tiles, :] = jnp.where(first, -ref, 0.0).astype(q_turned.dtype)
            p = jnp.where(own_allowed, jnp.exp2((s - ref) * rate), 0.0)
            total[t] = jnp.sum(p.reshape(piece // 8, 8, lanes), axis=0)
            v = v_turned[(core * RING + z) * ROW + at]
            acc[t] = jnp.dot(v[:, b * piece:(b + 1) * piece], p.astype(jnp.bfloat16), preferred_element_type=jnp.float32)

    take(x, c)
    arrived(q_all.at[x, 1 - c], q_recv.at[steps.index((0, 1))])
    take(x, 1 - c)

    def await_queries(dx):
        for core in range(2):
            if dx == 2:
                for side in range(2):
                    dc = (core + c) % 2
                    arrived(q_all.at[(x + 2) % ROW, core, side], on_recv.at[side, dc])
            else:
                dc = (core + c) % 2
                arrived(q_all.at[(x + ROW - dx) % ROW, core], q_recv.at[steps.index((dx, 0)) + dc])

    def row_at(n):
        off = jnp.where(n % 2 == 1, -((n + 1) // 2), n // 2)
        return off, (z + off + RING) % RING

    def weigh(t, zc, buf):
        own = (t // EACH % 2 * ROW + t // (2 * EACH)) * EACH + t % EACH
        before = place_ref[zc] < place_ref[z, pl.ds(own, 1), :]
        q_turned[t, width:width + tiles, :] = jnp.where(before, 0.0, -NEVER).astype(q_turned.dtype)
        k = [kv_all[core, zc, at, 0].reshape(EACH * piece, width) for core in range(2) for at in range(ROW)]
        keys = jnp.concatenate([jnp.concatenate(k, axis=0), marks[...]], axis=1)
        s = jnp.dot(keys, q_turned[t], preferred_element_type=jnp.float32)
        p = jnp.exp2(s * rate)
        total[t] += jnp.sum(p.reshape(window // 8, 8, lanes), axis=0)
        p_bufs[buf][...] = p.astype(jnp.bfloat16)

    def absorb(t, zc, buf):
        v = [v_turned[(core * RING + zc) * ROW + at] for core in range(2) for at in range(ROW)]
        acc[t] += jnp.dot(jnp.concatenate(v, axis=1), p_bufs[buf][...], preferred_element_type=jnp.float32)

    def rise(t, j):
        slot = slot_of(-t, j)
        arrived(slot, up_recv.at[t - 1, j])

        @pl.when((t < 3) | ((t == 3) & (j < 2)))
        def _():
            pass_up(t, j, slot)

        to_partner(-t, j, slot)

    def fall(t, j):
        slot = slot_of(t, j)
        arrived(slot, down_recv.at[t - 1, j])

        @pl.when((t < 3) | ((t == 3) & (j >= 2)))
        def _():
            pass_down(t, j, slot)

        to_partner(t, j, slot)

    for j in (0, 1, 3, 2):
        rise(1, j)
        fall(1, j)

    per_turn = 2 * EACH
    turns = ROW * NEAR

    def plan(m):
        g = m // NEAR
        chip = (x + jnp.where(g == 1, 3, jnp.where(g == 2, 1, jnp.where(g == 3, 2, 0)))) % ROW
        return chip, chip * per_turn, row_at(m % NEAR)[1]

    def hop(event):
        t, j = event // ROW + 2, event % ROW
        j = jnp.where(j == 2, 3, jnp.where(j == 3, 2, j))
        rise(t, j)
        fall(t, j)

    def turn(m, carry):
        _, base, zc = plan(m)
        chip, next_base, next_zc = plan(m + 1)

        @pl.when(m < NEAR - 1)
        def _():
            ready(next_zc)

        @pl.when((m >= NEAR - 1) & (m <= 3 * NEAR - 1))
        def _():
            hop(m - NEAR + 1 + jnp.where(m > 2 * NEAR, 1, 0))

        @pl.when(m == 2 * NEAR)
        def _():
            hop(m - NEAR + 2)

        @pl.when(m == turns - 2)
        def _():
            rise(RING // 2, 0)
            fall(RING // 2, 3)

        for g, dx in ((1, 1), (2, 3), (3, 2)):
            @pl.when(m == NEAR * g - 1)
            def _(dx=dx):
                await_queries(dx)

        @pl.when(m == NEAR + 1)
        def _():
            forward()

        @pl.when((m == NEAR - 1) | (m == 2 * NEAR - 1) | (m == 3 * NEAR - 1))
        def _():
            take(chip, 0)
            take(chip, 1)

        for u in range(per_turn):
            done = u == per_turn - 1
            weigh(next_base if done else base + u + 1, next_zc if done else zc, 1 - u % 2)
            absorb(base + u, zc, u % 2)
        return carry

    weigh(x * per_turn, z, 0)
    lax.fori_loop(0, turns - 1, turn, 0)
    rise(RING // 2, 1)
    fall(RING // 2, 2)
    _, last_base, last_zc = plan(turns - 1)
    for u in range(per_turn):
        if u < per_turn - 1:
            weigh(last_base + u + 1, last_zc, 1 - u % 2)
        absorb(last_base + u, last_zc, u % 2)
    for r in range(2, RING - 1):
        for j in range(ROW):
            arrived(kv_all.at[1 - c, (z + r) % RING, (x + j) % ROW], core_recv.at[r, j])

    for j in range(ROW):
        for t in range(RING // 2):
            if t < 3 or j < 2:
                gone(slot_of(0, j), up_send.at[t, j])
            if t < 3 or j >= 2:
                gone(slot_of(0, j), down_send.at[t, j])
        for r in range(RING):
            gone(slot_of(0, j), core_send.at[r, j])
        if j:
            gone(slot_of(0, j), x_send.at[j])
    for side in range(2):
        for dc in range(2):
            gone(relay.at[side, dc], far_send.at[side, dc])
            gone(relay.at[side, dc], on_send.at[side, dc])
    for n, (dx, dc) in enumerate(steps):
        if dx != 2:
            gone(q_all.at[x, c], q_send.at[n])


def attend(order, q, kv):
    sem = pltpu.SemaphoreType.DMA
    half_ring = RING // 2
    vmem = pl.BlockSpec(memory_space=pltpu.VMEM)
    lanes, width = q.shape[-2:]
    piece = kv.shape[-2]
    tiles = 2 * ROW * EACH
    window = tiles * piece
    return pl.pallas_call(
        attend_kernel,
        out_shape=(jax.ShapeDtypeStruct((ROW, 2, *q.shape[2:]), q.dtype),
                   jax.ShapeDtypeStruct((2, RING, ROW, *kv.shape[1:]), kv.dtype),
                   jax.ShapeDtypeStruct((tiles, width, lanes), jnp.float32),
                   jax.ShapeDtypeStruct((tiles, 8, lanes), jnp.float32),
                   jax.ShapeDtypeStruct((tiles, 1, lanes), jnp.float32),
                   jax.ShapeDtypeStruct((tiles, 2 * width, lanes), jnp.bfloat16),
                   jax.ShapeDtypeStruct((window, width), jnp.bfloat16)),
        in_specs=[pl.BlockSpec(memory_space=pltpu.SMEM), vmem, vmem],
        out_specs=(vmem,) * 7,
        scratch_shapes=[
            pltpu.VMEM((RING, tiles, lanes), jnp.int32),
            pltpu.VMEM((2 * RING * ROW, width, width), jnp.bfloat16),
            [pltpu.VMEM((window, lanes), jnp.bfloat16)] * 2,
            pltpu.VMEM((2, 2, lanes, width), jnp.bfloat16),
            sem((2 * ROW - 1,)), sem((2 * ROW - 1,)), sem((2, 2)), sem((2, 2)), sem((2, 2)), sem((2, 2)),
            sem((ROW,)), sem((ROW,)),
            sem((half_ring, ROW)), sem((half_ring, ROW)), sem((half_ring, ROW)), sem((half_ring, ROW)),
            sem((RING, ROW)), sem((RING, ROW)), sem((2,)),
        ],
        compiler_params=pltpu.CompilerParams(
            collective_id=0, has_side_effects=True, vmem_limit_bytes=32 * 1024 * 1024),
        cost_estimate=pl.CostEstimate(flops=10**10, bytes_accessed=20_000_000, transcendentals=0),
    )(order, q, kv)


def finish_kernel(order, rank, q_all, kv_all, acc, total, top, q_turned, marks, o_ref, lse_ref,
                  k_sorted, v_sorted, v_turned, p_bufs, far_acc, far_total, again_acc, again_top):
    x, z, _, _ = place()
    half = x // 2
    tiles, _, lanes = acc.shape
    piece, width = kv_all.shape[-2:]
    block = 2 * piece
    rate = math.log2(math.e) / math.sqrt(width)
    q_row = lax.broadcasted_iota(jnp.int32, (1, lanes), 1) % block

    def put(t, weight, sums, reference):
        some = weight > 0
        weight = jnp.where(some, weight, 1.0)
        o_ref[t] = (sums * (1.0 / weight)).astype(jnp.bfloat16).T
        lse_ref[t] = jnp.where(some, reference + jnp.log2(weight), -1e30)

    window = marks.shape[0]
    per_window = window // piece

    def sort(i, carry):
        n, g = i // (2 * ROW), i % (2 * ROW)
        off = jnp.where(n % 2 == 1, (n + 3) // 2, -((n + 4) // 2))
        zc = (z + off + RING) % RING
        core, at_x = g // ROW, g % ROW
        for b in range(EACH):
            at = pl.multiple_of(rank[stored(zc, core, at_x, b)] * piece, piece)
            k_sorted[pl.ds(at, piece), :] = kv_all[core, zc, at_x, 0, b]
            v_sorted[pl.ds(at, piece), :] = kv_all[core, zc, at_x, 1, b]
        return carry

    lax.fori_loop(0, (RING - NEAR) * 2 * ROW, sort, 0, unroll=4)

    def turn(g, carry):
        at = pl.multiple_of(g * width, width)
        v_turned[g] = v_sorted[pl.ds(at, width), :].T
        return carry

    lax.fori_loop(0, v_turned.shape[0], turn, 0, unroll=8)

    def own_block(t):
        return stored(z, t // EACH % 2, t // (2 * EACH), t % EACH)

    def count_of(t):
        held = rank[own_block(jnp.minimum(t, tiles - 1))]
        return jnp.where(t < tiles, held, 0)

    def clear(t, items):
        far_acc[t] = jnp.zeros(far_acc.shape[1:], jnp.float32)
        far_total[t] = jnp.zeros(far_total.shape[1:], jnp.float32)
        return items + jnp.maximum((count_of(t) + per_window - 1) // per_window, 1)

    items = lax.fori_loop(0, tiles, clear, 0)
    block_row = lax.broadcasted_iota(jnp.int32, (tiles, lanes), 0)

    def weigh(t, w, buf):
        count, t = count_of(t), jnp.minimum(t, tiles - 1)
        at = pl.multiple_of(w * window, window)
        mask = jnp.where(block_row < count - w * per_window, 0.0, -NEVER).astype(q_turned.dtype)
        right = jnp.concatenate([q_turned[t, :width, :], mask, q_turned[t, width + tiles:, :]], axis=0)
        keys = jnp.concatenate([k_sorted[pl.ds(at, window), :], marks[...]], axis=1)
        p = jnp.exp2(jnp.dot(keys, right, preferred_element_type=jnp.float32) * rate)
        far_total[t] += jnp.sum(p.reshape(window // 8, 8, lanes), axis=0)
        p_bufs[buf][...] = p.astype(jnp.bfloat16)

    def absorb(t, w, buf):
        t = jnp.minimum(t, tiles - 1)
        v = [v_turned[w * (window // width) + i] for i in range(window // width)]
        far_acc[t] += jnp.dot(jnp.concatenate(v, axis=1), p_bufs[buf][...], preferred_element_type=jnp.float32)

    unroll = 4

    def step(i, at):
        t, w = at
        for u in range(unroll):
            last = (w + 1) * per_window >= count_of(t)
            next_t, next_w = jnp.where(last, t + 1, t), jnp.where(last, 0, w + 1)
            weigh(next_t, next_w, 1 - u % 2)
            absorb(t, w, u % 2)
            t, w = next_t, next_w
        return t, w

    weigh(jnp.int32(0), jnp.int32(0), 0)
    lax.fori_loop(0, (items + unroll - 1) // unroll, step, (jnp.int32(0), jnp.int32(0)))

    worst = jnp.zeros((1, lanes), jnp.float32)
    for t in range(tiles):
        weight = jnp.sum(total[t] + far_total[t], axis=0, keepdims=True)
        no_key = q_row < jnp.where(order[own_block(t)] == 0, half * piece, 0)
        fits = ((weight > 2.0**-60) & (weight < 2.0**80)) | no_key
        worst = jnp.maximum(worst, jnp.where(fits, 0.0, 1.0))
        put(t, weight, acc[t] + far_acc[t], top[t] * rate)

    def redo(t, carry):
        at_q, core_q, b_q = t // (2 * EACH), t // EACH % 2, t % EACH
        pos = order[stored(z, core_q, at_q, b_q)]
        q = q_all[at_q, core_q, b_q].T
        again_acc[...] = jnp.zeros_like(again_acc)
        again_top[0:1, :] = jnp.full((1, lanes), -1e30, jnp.float32)
        again_top[1:2, :] = jnp.zeros((1, lanes), jnp.float32)

        def one(g, carry):
            core, zc, at = g // (RING * ROW), g // ROW % RING, g % ROW
            for b in range(EACH):
                kp = order[stored(zc, core, at, b)]
                k_at = lax.broadcasted_iota(jnp.int32, (piece, lanes), 0) + half * piece + kp * block
                s = jnp.dot(kv_all[core, zc, at, 0, b], q, preferred_element_type=jnp.float32) * rate
                s = jnp.where(k_at <= pos * block + q_row, s, -2e30)
                old = again_top[0:1, :]
                new = jnp.maximum(old, jnp.max(s, axis=0, keepdims=True))
                p = jnp.exp2(s - new)
                fade = jnp.exp2(old - new)
                again_top[0:1, :] = new
                again_top[1:2, :] = again_top[1:2, :] * fade + jnp.sum(p, axis=0, keepdims=True)
                v = kv_all[core, zc, at, 1, b].T
                again_acc[...] = again_acc[...] * fade + jnp.dot(
                    v, p.astype(jnp.bfloat16), preferred_element_type=jnp.float32)
            return carry

        lax.fori_loop(0, 2 * RING * ROW, one, 0)
        put(t, again_top[1:2, :], again_acc[...], again_top[0:1, :])
        return carry

    @pl.when(jnp.max(worst) > 0)
    def _():
        lax.fori_loop(0, tiles, redo, 0)


def finish(order, rank, q_all, kv_all, acc, total, top, q_turned, marks):
    smem = pl.BlockSpec(memory_space=pltpu.SMEM)
    vmem = pl.BlockSpec(memory_space=pltpu.VMEM)
    tiles, width, lanes = acc.shape
    far = (RING - NEAR) * 2 * ROW * EACH * kv_all.shape[-2]
    return pl.pallas_call(
        finish_kernel,
        out_shape=(jax.ShapeDtypeStruct((tiles, lanes, width), jnp.bfloat16),
                   jax.ShapeDtypeStruct((tiles, 1, lanes), jnp.float32)),
        in_specs=[smem, smem, *[vmem] * 7],
        out_specs=(vmem, vmem),
        scratch_shapes=[
            pltpu.VMEM((far, width), jnp.bfloat16),
            pltpu.VMEM((far, width), jnp.bfloat16),
            pltpu.VMEM((far // width, width, width), jnp.bfloat16),
            [pltpu.VMEM((marks.shape[0], lanes), jnp.bfloat16)] * 2,
            pltpu.VMEM(acc.shape, jnp.float32),
            pltpu.VMEM(total.shape, jnp.float32),
            pltpu.VMEM((width, lanes), jnp.float32),
            pltpu.VMEM((8, lanes), jnp.float32),
        ],
        compiler_params=pltpu.CompilerParams(vmem_limit_bytes=28 * 1024 * 1024),
    )(order, rank, q_all, kv_all, acc, total, top, q_turned, marks)


def return_kernel(o_ref, lse_ref, o_all, lse_all, relay, o_send, o_recv, l_send, l_recv,
                  far_send, far_recv, on_send, on_recv, own_sem):
    x, z, c, y = place()
    steps, mates = row_mates(x, z, c, y)
    mate = dict(zip(steps, mates))
    greet(mates)
    keep = [pltpu.make_async_copy(o_ref.at[x, c], o_all.at[x, c], own_sem.at[0]),
            pltpu.make_async_copy(lse_ref.at[x, c], lse_all.at[x, c], own_sem.at[1])]
    copies, far = [], []
    for side, dx in ((0, 1), (1, 3)):
        for dc in range(2):
            far.append(remote(o_ref.at[(x + 2) % ROW, (c + dc) % 2, side], relay.at[side, dc],
                              far_send.at[side, dc], far_recv.at[side, dc], mate[dx, 0]))
            far[-1].start()
    for n, (dx, dc) in enumerate(steps):
        to_x, to_c = (x + dx) % ROW, (c + dc) % 2
        copies.append(remote(lse_ref.at[to_x, to_c], lse_all.at[x, c], l_send.at[n], l_recv.at[n], mates[n]))
        copies[-1].start()
        if dx != 2:
            copies.append(remote(o_ref.at[to_x, to_c], o_all.at[x, c], o_send.at[n], o_recv.at[n], mates[n]))
            copies[-1].start()
    for copy in keep:
        copy.start()
    for k, (side, dx) in enumerate(((0, 1), (1, 3))):
        for dc in range(2):
            far[2 * k + dc].wait()
            copies.append(remote(relay.at[side, dc], o_all.at[(x + ROW - dx) % ROW, c, side],
                                 on_send.at[side, dc], on_recv.at[side, dc], mate[dx, dc]))
            copies[-1].start()
    for copy in [*keep, *copies]:
        copy.wait()


def send_back(o, lse):
    sem = pltpu.SemaphoreType.DMA
    vmem = pl.BlockSpec(memory_space=pltpu.VMEM)
    n = 2 * ROW - 1
    return pl.pallas_call(
        return_kernel,
        out_shape=(jax.ShapeDtypeStruct(o.shape, o.dtype), jax.ShapeDtypeStruct(lse.shape, lse.dtype)),
        in_specs=[vmem, vmem],
        out_specs=(vmem, vmem),
        scratch_shapes=[pltpu.VMEM((2, 2, *o.shape[-2:]), o.dtype),
                        sem((n,)), sem((n,)), sem((n,)), sem((n,)),
                        sem((2, 2)), sem((2, 2)), sem((2, 2)), sem((2, 2)), sem((2,))],
        compiler_params=pltpu.CompilerParams(
            collective_id=1, has_side_effects=True, vmem_limit_bytes=32 * 1024 * 1024),
        cost_estimate=pl.CostEstimate(flops=0, bytes_accessed=20_000_000, transcendentals=0),
    )(o, lse)


def body(stored_query_rows, stored_key_rows, stored_value_rows, span_order):
    rows, heads, width = stored_query_rows.shape
    span = rows // EACH
    q = stored_query_rows.reshape(EACH, span, 2, 2, 2, width).transpose(2, 3, 0, 4, 1, 5)
    q = q.reshape(2, 2, EACH, 2 * span, width)
    kv = jnp.stack([stored_key_rows, stored_value_rows])
    kv = kv.reshape(2, EACH, 2, span // 2, 2, width).transpose(4, 2, 0, 1, 3, 5)
    kv = kv.reshape(4, 2, EACH, span // 2, width)
    block = jnp.arange(span_order.shape[0])
    row = block // (2 * RING * EACH) * 2 + block // EACH % 2
    away = (row - place()[1] + RING + NEAR // 2) % RING >= NEAR
    rank = jnp.sum((away[None, :] & (span_order[None, :] < span_order[:, None])).astype(jnp.int32), axis=1)
    o, lse = finish(span_order, rank, *attend(span_order, q, kv))

    o, lse = send_back(o.reshape(ROW, 2, EACH, 2 * span, width), lse.reshape(ROW, 2, EACH, 1, 2 * span))
    o = o.reshape(2, 2, 2, EACH, 2, span, width)
    lse = lse.reshape(2, 2, 2, EACH, 2, span)
    top = jnp.max(lse, axis=0)
    weights = jnp.exp2(lse - top)
    share = weights / jnp.sum(weights, axis=0)
    result = jnp.sum(o.astype(jnp.float32) * share[..., None], axis=0).astype(jnp.bfloat16)
    return result.transpose(2, 4, 0, 1, 3, 5).reshape(rows, heads, width)


def solution(mesh):
    placed = (
        P(("outer", "inner"), "head", None),
        P(("outer", "inner"), "head", None),
        P(("outer", "inner"), "head", None),
        P(),
    )
    return jax.shard_map(
        body,
        mesh=mesh,
        in_specs=placed,
        out_specs=P(("outer", "inner"), "head", None),
        check_vma=False,
    )
```
